32 devices in a mesh: rows: 8 (over z, x), grp: 4 (over y, core).
Axes of the slice: x: 2, y: 2, z: 4, core: 2. Of those that a mesh axis runs over, the one named last changes fastest.
Arguments:
- matrix: bfloat16 [10240, 16384], P(('rows', 'grp')), may hold values from -36 to 36
- sample_rows: int32 [32, 128, 256], P(('rows', 'grp')), may hold values from 0 to 319
- pair_list: int32 [8, 8, 4], replicated, may hold values from 0 to 255, as said below
- pair_count: int32 [8, 8], replicated, may hold values from 1 to 4, as said below
- pair_blocks: int32 [256, 2], replicated, may hold values from 0 to 127, as said below
Outputs:
- gram: float32 [256, 128, 128], P(('rows', 'grp'))
The draws below stay inside these ranges and needn't reach their ends.
Inputs may be any that keep to these rules, and one draw needn't show every extreme that they name: `pair_list`: entry [s, r, k] lies in [r * 32, (r + 1) * 32); the 4 entries of one [s, r] are distinct. `pair_count`: every row group has some owner with all 4 slots active, and some owner has all 4 slots active from every row group. `pair_blocks`: the two blocks of a pair differ.
All inputs are finite; a program needn't handle non-finite values.
Results may differ from the reference program's by a relative error of at most 0.0016.
Values sent between devices are 32-bit elements; how exact they have to be, the bound alone decides.
A program may use at most 192 MiB of HBM per device.

```python
import math
import jax
import jax.numpy as jnp
from jax import lax

BLOCK = 128
NB = 128
ROWS_DEV = 320
SAMP = 256
CAP = 4
NCOL = 16384
ROWS_TOTAL = 10240
PAIRS = 256
REGION = 32
N_ROWS = 8
N_GRP = 4
DEVICES = 32


def draw_matrix(key, part):
    key_base, key_row, key_col = jax.random.split(key, 3)
    row_scale = jnp.exp(jax.random.uniform(key_row, (ROWS_TOTAL, 1), jnp.float32, math.log(0.3), math.log(3.0)))
    col_scale = jnp.exp(jax.random.uniform(key_col, (1, NCOL), jnp.float32, math.log(0.5), math.log(2.0)))
    base = jnp.clip(jax.random.normal(key_base, (ROWS_TOTAL, NCOL), jnp.float32), -6.0, 6.0)
    return (base * row_scale * col_scale).astype(jnp.bfloat16)


def draw_pair_list(key, part):
    keys = jax.random.split(jax.random.fold_in(key, 11), N_ROWS * N_ROWS)
    chosen = jax.vmap(lambda single: jax.random.permutation(single, REGION)[:CAP])(keys)
    chosen = chosen.reshape(N_ROWS, N_ROWS, CAP).astype(jnp.int32)
    owner_base = (jnp.arange(N_ROWS, dtype=jnp.int32) * REGION)[None, :, None]
    return chosen + owner_base


def draw_pair_count(key, part):
    key_count, key_row, key_col = jax.random.split(jax.random.fold_in(key, 23), 3)
    counts = jax.random.randint(key_count, (N_ROWS, N_ROWS), 1, CAP + 1).astype(jnp.int32)
    full_owner = jax.random.randint(key_row, (N_ROWS,), 0, N_ROWS)
    counts = counts.at[jnp.arange(N_ROWS), full_owner].set(CAP)
    common_owner = jax.random.randint(key_col, (), 0, N_ROWS)
    counts = counts.at[:, common_owner].set(CAP)
    return counts.astype(jnp.int32)


def draw_pair_blocks(key, part):
    key_first, key_step = jax.random.split(jax.random.fold_in(key, 37))
    first_block = jax.random.randint(key_first, (PAIRS,), 0, NB)
    step_size = jax.random.randint(key_step, (PAIRS,), 1, NB)
    second_block = (first_block + step_size) % NB
    return jnp.stack([first_block, second_block], axis=1).astype(jnp.int32)


def touch_ends(result, rng, smallest, high):
    dims = result.shape
    place = [jax.random.randint(jax.random.fold_in(rng, axis), (), 0, dims[axis]) for axis in range(len(dims))]
    result = result.at[tuple(place)].set(smallest)
    longest = dims.index(max(dims))
    place[longest] = (place[longest] + 1) % dims[longest]
    return result.at[tuple(place)].set(high)


def setup_inputs(seed: int = 0) -> dict:
    seeds = jax.random.split(jax.random.key(seed), 6)
    return {
        "matrix": draw_matrix(jax.random.fold_in(seeds[5], 71), 0),
        "sample_rows": touch_ends(jax.random.randint(seeds[1], (DEVICES, NB, SAMP), 0, ROWS_DEV), jax.random.fold_in(seeds[1], 1), 0, ROWS_DEV - 1).astype(jnp.int32),
        "pair_list": draw_pair_list(jax.random.fold_in(seeds[5], 71), 0),
        "pair_count": draw_pair_count(jax.random.fold_in(seeds[5], 71), 0),
        "pair_blocks": draw_pair_blocks(jax.random.fold_in(seeds[5], 71), 0),
    }


def reference(matrix, sample_rows, pair_list, pair_count, pair_blocks):
    device_total = N_ROWS * N_GRP
    blocks_all = matrix.reshape(device_total, ROWS_DEV, NB, BLOCK)
    positions = jnp.arange(ROWS_DEV, dtype=jnp.int32)
    slot_numbers = jnp.arange(CAP, dtype=jnp.int32)

    def one_device(raw_tiles, device):
        source = device // N_GRP
        blocks = blocks_all[device]
        picked = sample_rows[device]
        multiplicity = lax.optimization_barrier(jnp.sum((picked[:, :, None] == positions[None, None, :]).astype(jnp.float32), axis=1))
        weighted = (jnp.transpose(multiplicity)[:, :, None] * blocks.astype(jnp.float32)).astype(jnp.bfloat16)
        pair_ids = pair_list[source].reshape(-1)
        live_mask = (slot_numbers[None, :] < pair_count[source][:, None]).reshape(-1).astype(jnp.float32)
        first_block = pair_blocks[pair_ids, 0]
        second_block = pair_blocks[pair_ids, 1]
        weighted_cols = jnp.take(weighted, first_block, axis=1).astype(jnp.float32)
        plain_cols = jnp.take(blocks, second_block, axis=1).astype(jnp.float32)
        partial_tiles = jnp.einsum('rgi,rgj->gij', weighted_cols, plain_cols)
        partial_tiles = partial_tiles * live_mask[:, None, None]
        return (raw_tiles.at[pair_ids].add(partial_tiles), None)
    start = jnp.zeros((PAIRS, BLOCK, BLOCK), jnp.float32)
    raw_tiles, _ = lax.scan(one_device, start, jnp.arange(device_total, dtype=jnp.int32))
    squares = lax.optimization_barrier(jnp.sum(jnp.square(matrix.astype(jnp.float32)), axis=0))
    root_mean = jnp.sqrt(squares / ROWS_TOTAL + 1e-06).reshape(NB, BLOCK)
    left_scale = root_mean[pair_blocks[:, 0]]
    right_scale = root_mean[pair_blocks[:, 1]]
    return raw_tiles / (SAMP * left_scale[:, :, None] * right_scale[:, None, :])
```

```python
import functools

import jax
import jax.numpy as jnp
from jax import lax
from jax.experimental import pallas as pl
from jax.experimental.pallas import tpu as pltpu
from jax.sharding import PartitionSpec as P

epsilon = 1e-06
MESH = pl.DeviceIdType.MESH
F32 = jnp.float32
BF16 = jnp.bfloat16
CHUNKS = 4
LOADS = 8
FOLD_LAG = 3
CROSS_LAG = 6
EARLY = 6
scope = jax.named_scope


def kernel(
    dims, list_hbm, count_hbm, blocks_hbm, samples_hbm, matrix, out, *scratch,
):
    row_count, grp_count, cap, pairs, pre = dims
    it = iter(scratch)
    mat, samples, counts, places, tiles, core_in, high_in = [next(it) for _ in range(7)]
    row_in = [next(it) for _ in range(CHUNKS)]
    part_b, in_b, held, part_c, in_c, scale = [next(it) for _ in range(6)]
    squares, sq_in, sq_half, sq_in2, sq_rows, sq_sum, sq_far, sq_total = [next(it) for _ in range(8)]
    pair_list, pair_count, pair_blocks = [next(it) for _ in range(3)]
    (table_sem, sample_sem, load_sem, sq_send, sq_recv, near_send, near_recv, core_send, core_recv,
     high_send, high_recv, row_send, row_recv, b_send, b_recv, c_send, c_recv) = it

    block_count, rows_dev, width = mat.shape
    sample_count = samples.shape[1]
    half = cap // 2
    region = pairs // row_count
    tile_dev = region // grp_count
    row_half = row_count // 2
    tall = width // 2
    thin = tall // CHUNKS

    s = lax.axis_index("rows")
    g = lax.axis_index("grp")
    low = lax.rem(g, 2)
    high = lax.div(g, 2)
    partner = high * 2 + (1 - low)
    across = (1 - high) * 2 + low

    def send(source, target, send_sem, recv_sem, row, grp):
        return pltpu.make_async_remote_copy(
            src_ref=source, dst_ref=target, send_sem=send_sem, recv_sem=recv_sem,
            device_id={"rows": row, "grp": grp}, device_id_type=MESH,
        )

    def await_bytes(ref, sem):
        pltpu.make_async_copy(ref, ref, sem).wait()

    def lines_from(start, size):
        return pl.ds(pl.multiple_of(start, 8), size)

    with scope("greet"):
        barrier = pltpu.get_barrier_semaphore()
        pl.semaphore_signal(barrier, inc=1, device_id={"rows": s, "grp": partner}, device_id_type=MESH)
        pl.semaphore_signal(barrier, inc=1, device_id={"rows": s, "grp": across}, device_id_type=MESH)

        def greet(j, carry):
            row = lax.rem(s + j, row_count)
            pl.semaphore_signal(barrier, inc=1, device_id={"rows": row, "grp": g}, device_id_type=MESH)
            return carry

        lax.fori_loop(1, row_count, greet, 0)

    batch = block_count // LOADS

    def load_go(i, carry):
        source = matrix.at[:, pl.ds(pl.multiple_of(i * width, width), width)]
        pltpu.make_async_copy(source, mat.at[i], load_sem.at[lax.div(i, batch)]).start()
        return carry

    with scope("issue"):
        tables = [
            pltpu.make_async_copy(source, target, table_sem.at[n])
            for n, (source, target) in enumerate(
                ((list_hbm, pair_list), (count_hbm, pair_count), (blocks_hbm, pair_blocks))
            )
        ]
        sample_load = pltpu.make_async_copy(samples_hbm, samples, sample_sem)
        sample_load.start()
        for table in tables:
            table.start()
        lax.fori_loop(0, block_count, load_go, 0)

    top = lax.div(s, row_half)

    def owner_of(k):
        other = 1 - lax.div(k, row_half)
        j = k + 1 - other
        return (top * (1 - other) + (1 - top) * other) * row_half + lax.rem(s + j, row_half)

    zero_tile = jnp.zeros((thin, width), F32)

    def clear(j, carry):
        for q in range(CHUNKS):
            row_in[q][j, cap] = zero_tile
        return carry

    lax.fori_loop(0, row_count, clear, 0)

    def source_of(k):
        return ((1 - top) if k < row_half else top) * row_half + lax.rem(s + k, row_half)

    def place(j, carry):
        pair = s * region + j
        for k in range(row_count):
            source = source_of(k)
            slot = cap
            for n in range(half if k < row_half else cap):
                at = high * half + n if k < row_half else n
                slot = jnp.where(pair_list[source, at, s] == pair, at, slot)
            places[j, k] = slot
        return carry

    with scope("w_samples"):
        sample_load.wait()
        for table in tables:
            table.wait()

    positions = lax.broadcasted_iota(jnp.int32, (rows_dev, sample_count), 0)
    ones = jnp.ones((sample_count, width), BF16)

    def count(owner, slot):
        first = pair_blocks[0, pair_list[s, slot, owner]]
        active = (slot < pair_count[s, owner]).astype(F32)
        picked = samples[first].reshape(1, sample_count)
        hits = jnp.where(positions == picked, 1.0, 0.0).astype(BF16)
        multiplicity = jnp.dot(hits, ones, preferred_element_type=F32)
        return (multiplicity * active).astype(BF16)

    def count_owner(k, carry):
        owner = owner_of(k)
        for n in range(cap):
            counts[lax.rem(k, pre), n] = count(owner, n)
        return carry

    with scope("counts"):
        lax.fori_loop(0, pre, count_owner, 0)

    def square_group(n, carry):
        lines = []
        for m in range(8):
            values = mat[n * 8 + m].astype(F32)
            lines.append(jnp.sum(values * values, axis=0, keepdims=True))
        squares[lines_from(n * 8, 8), :] = jnp.concatenate(lines, axis=0)
        return carry

    with scope("load_sq"):
        for i in range(LOADS):
            with scope("w_load"):
                await_bytes(mat.at[pl.ds(i * batch, batch)], load_sem.at[i])
            if i < EARLY:
                lax.fori_loop(i * batch // 8, (i + 1) * batch // 8, square_group, 0)

    nb2 = block_count // 2
    nb4 = block_count // 4
    my_half = lines_from(low * nb2, nb2)
    quarter = lines_from(low * nb2 + high * nb4, nb4)

    sq1 = send(squares.at[lines_from((1 - low) * nb2, nb2)], sq_in, sq_send.at[0], sq_recv.at[0], s, partner)
    sq2 = send(sq_half.at[lines_from((1 - high) * nb4, nb4)], sq_in2, sq_send.at[1], sq_recv.at[1], s, across)
    sq4 = send(sq_total.at[quarter], sq_total.at[quarter], sq_send.at[2], sq_recv.at[2], s, across)
    sq5 = send(sq_total.at[my_half], sq_total.at[my_half], sq_send.at[3], sq_recv.at[3], s, partner)

    def near_row(j):
        return top * row_half + lax.rem(s + j, row_half)

    def sq_near(j):
        return send(sq_rows.at[s], sq_rows.at[s], near_send, near_recv, near_row(j), g)

    def sq_near_go(j, carry):
        sq_near(j).start()
        return carry

    sq3 = send(sq_sum, sq_far, sq_send.at[4], sq_recv.at[4], (1 - top) * row_half + lax.rem(s, row_half), g)

    def sq_first():
        sq1.wait()
        sq_half[...] = squares[my_half, :] + sq_in[...]
        sq2.start()

    def sq_second():
        sq2.wait()
        sq_rows[s] = sq_half[lines_from(high * nb4, nb4), :] + sq_in2[...]
        lax.fori_loop(1, row_half, sq_near_go, 0)

    def sq_third():
        await_bytes(sq_rows.at[pl.ds(0, row_half - 1)], near_recv)
        total = sq_rows[near_row(0)]
        for j in range(1, row_half):
            total = total + sq_rows[near_row(j)]
        sq_sum[...] = total
        sq3.start()

    def sq_next():
        sq3.wait()
        sq_total[quarter, :] = sq_sum[...] + sq_far[...]
        sq4.start()

    def sq_fourth():
        sq4.wait()
        sq5.start()

    my_lines = lines_from(low * tall, tall)
    their_lines = lines_from((1 - low) * tall, tall)
    mine = pl.ds(high * half, half)
    theirs = pl.ds((1 - high) * half, half)
    every = pl.ds(0, cap)

    def lines(q):
        return lines_from(low * tall + q * thin, thin)

    def core_copy(k):
        return send(tiles.at[k, every, their_lines], core_in.at[k], core_send, core_recv.at[k], s, partner)

    def high_copy(k, q):
        target = high_in.at[k, pl.ds(0, half), pl.ds(q * thin, thin)]
        return send(tiles.at[k, theirs, lines(q)], target, high_send, high_recv.at[k * CHUNKS + q], s, across)

    def far_copy(k, q):
        return send(tiles.at[k, mine, lines(q)], row_in[q].at[s, mine], row_send, row_recv.at[q], owner_of(k), g)

    def near_copy(k, q):
        return send(tiles.at[k, every, lines(q)], row_in[q].at[s, every], row_send, row_recv.at[q], owner_of(k), g)

    def make(k):
        owner = owner_of(k)
        for n in range(cap):
            pair = pair_list[s, n, owner]
            left = mat[pair_blocks[0, pair]]
            right = mat[pair_blocks[1, pair]]
            weighted = counts[lax.rem(k, pre), n] * left
            tiles[k, n] = lax.dot_general(
                weighted, right, (((0,), (0,)), ((), ())), preferred_element_type=F32
            )

    def fold(k):
        core_copy(k).wait_recv()
        tiles[k, :, my_lines] = tiles[k, :, my_lines] + core_in[k]

    def cross(k, q):
        high_copy(k, q).wait_recv()
        tiles[k, mine, lines(q)] = tiles[k, mine, lines(q)] + high_in[k, :, pl.ds(q * thin, thin)]
        far_copy(k, q).start()

    last = row_count - 1
    with scope("make"):
        make(0)
    with scope("barrier"):
        pl.semaphore_wait(barrier, row_count + 1)
    core_copy(0).start()

    def step(i, carry):
        @pl.when(i < pre)
        def _():
            with scope("make"):
                make(i)
            core_copy(i).start()

        @pl.when(i == row_half)
        def _():
            with scope("squares"):
                lax.fori_loop(EARLY * batch // 8, block_count // 8, square_group, 0)
            sq1.start()

        if pre < row_count:
            @pl.when((i >= pre) & (i < row_count))
            def _():
                with scope("make_b"):
                    count_owner(i, 0)
                    make(i)
                core_copy(i).start()

        @pl.when(i == row_half + 2)
        def _():
            with scope("sq_first"):
                sq_first()

        k = i - FOLD_LAG

        @pl.when((k >= 0) & (k < row_count))
        def _():
            with scope("fold"):
                fold(k)

            @pl.when(k < row_half)
            def _():
                high_copy(k, 0).start()

            @pl.when(k == row_half - 1)
            def _():
                for q in range(1, CHUNKS):
                    def rest(j, carry):
                        high_copy(j, q).start()
                        return carry

                    lax.fori_loop(0, row_half, rest, 0)

            @pl.when((k >= row_half) & (k < last))
            def _():
                near_copy(k, 0).start()

        m = i - CROSS_LAG

        @pl.when((m >= 0) & (m < row_half))
        def _():
            with scope("cross"):
                cross(m, 0)

        return carry

    lax.fori_loop(1, max(row_count + FOLD_LAG, row_half + CROSS_LAG), step, 0)
    for q in range(1, CHUNKS):
        def near_go(k, carry):
            near_copy(k, q).start()
            return carry

        def cross_go(k, carry):
            cross(k, q)
            return carry

        lax.fori_loop(row_half, last, near_go, 0)
        with scope("crosses"):
            lax.fori_loop(0, row_half, cross_go, 0)
        if q == 1:
            with scope("sq_second"):
                sq_second()
    with scope("places"):
        lax.fori_loop(0, region, place, 0)
    for q in range(CHUNKS):
        row_in[q][s, every] = tiles[last, :, lines(q)]

    def owned(q, grp, n):
        j = grp * tile_dev + n
        total = row_in[q][source_of(0), places[j, 0]]
        for k in range(1, row_count):
            total = total + row_in[q][source_of(k), places[j, k]]
        return total

    distant = ((1 - high) * 2 + (1 - low), (1 - high) * 2 + low)
    local = (partner, g)

    def b_copy(q, t):
        k = q * 2 + t
        return send(part_b.at[q, t], in_b.at[q, t], b_send, b_recv.at[k], s, across)

    def c_copy(q):
        return send(part_c.at[q], in_c.at[q], c_send, c_recv.at[q], s, partner)

    arriving = 3 * row_count // 4 - 1

    def post(q):
        with scope("w_rows"):
            await_bytes(row_in[q].at[pl.ds(0, arriving), every], row_recv.at[q])
        with scope("post"):
            for t in range(2):
                def away(n, carry):
                    part_b[q, t, n] = owned(q, distant[t], n)
                    return carry

                lax.fori_loop(0, tile_dev, away, 0)
                b_copy(q, t).start()
            for t in range(2):
                def hold(n, carry):
                    held[q, t, n] = owned(q, local[t], n)
                    return carry

                lax.fori_loop(0, tile_dev, hold, 0)

    def finish(q, scaled):
        with scope("w_b0"):
            b_copy(q, 0).wait_recv()
        part_c[q] = held[q, 0] + in_b[q, 0]
        c_copy(q).start()
        with scope("w_b1"):
            b_copy(q, 1).wait_recv()
        here = lines(q)
        there = lines_from((1 - low) * tall + q * thin, thin)
        own = held[q, 1] + in_b[q, 1]
        out[:, here] = own * scale[:, here] if scaled else own
        with scope("w_c"):
            c_copy(q).wait_recv()
        out[:, there] = in_c[q] * scale[:, there] if scaled else in_c[q]

    def rescale():
        sq5.wait()
        sq_total[...] = jnp.sqrt(sq_total[...] / (rows_dev * row_count * grp_count) + epsilon)

        def factor(n, carry):
            pair = (s * region + g * tile_dev) + n
            left = sq_total[pair_blocks[0, pair]].reshape(1, width)
            right = sq_total[pair_blocks[1, pair]].reshape(1, width)
            left = jnp.broadcast_to(left, (width, width)).T
            scale[n] = 1.0 / (sample_count * left * right)
            return carry

        lax.fori_loop(0, tile_dev, factor, 0)
        for q in range(CHUNKS - 1):
            for side in range(2):
                piece = pl.ds(side * tall + q * thin, thin)
                out[:, piece] = out[:, piece] * scale[:, piece]

    post(0)
    with scope("sq_third"):
        sq_third()
    post(1)
    with scope("sq_next"):
        sq_next()
    finish(0, False)
    post(2)
    with scope("sq_fourth"):
        sq_fourth()
    finish(1, False)
    post(3)
    finish(2, False)
    with scope("rescale"):
        rescale()
    finish(3, True)

    with scope("drain"):
        await_bytes(core_in, core_send)
        await_bytes(high_in, high_send)
        await_bytes(tiles.at[pl.ds(0, arriving), every, pl.ds(0, tall)], row_send)
        await_bytes(part_b, b_send)
        await_bytes(part_c, c_send)
        await_bytes(sq_rows.at[pl.ds(0, row_half - 1)], near_send)


def shards(matrix, sample_rows, pair_list, pair_count, pair_blocks):
    rows_dev, column_count = matrix.shape
    block_count, sample_count = sample_rows.shape[1:]
    width = column_count // block_count
    row_count = lax.axis_size("rows")
    grp_count = lax.axis_size("grp")
    cap = pair_list.shape[2]
    pairs = pair_blocks.shape[0]
    region = pairs // row_count
    tile_dev = region // grp_count
    half = cap // 2
    row_half = row_count // 2
    tall = width // 2
    thin = tall // CHUNKS
    pre = min(row_half, 4)
    nb2, nb4 = block_count // 2, block_count // 4
    dma = pltpu.SemaphoreType.DMA

    def vmem(*shape):
        return pltpu.VMEM(shape, F32)

    return pl.pallas_call(
        functools.partial(kernel, (row_count, grp_count, cap, pairs, pre)),
        out_shape=pltpu.VMEM((tile_dev, width, width), F32),
        in_specs=[
            pl.BlockSpec(memory_space=pl.ANY) for _ in range(5)
        ],
        out_specs=pl.BlockSpec(memory_space=pltpu.VMEM),
        scratch_shapes=[
            pltpu.VMEM((block_count, rows_dev, width), BF16),
            pltpu.VMEM((block_count, sample_count), jnp.int32),
            pltpu.VMEM((pre, cap, rows_dev, width), BF16),
            pltpu.SMEM((region, row_count), jnp.int32),
            vmem(row_count, cap, width, width),
            vmem(row_count, cap, tall, width),
            vmem(row_half, half, tall, width),
            *[vmem(row_count, cap + 1, thin, width) for _ in range(CHUNKS)],
            vmem(CHUNKS, 2, tile_dev, thin, width),
            vmem(CHUNKS, 2, tile_dev, thin, width),
            vmem(CHUNKS, 2, tile_dev, thin, width),
            vmem(CHUNKS, tile_dev, thin, width),
            vmem(CHUNKS, tile_dev, thin, width),
            vmem(tile_dev, width, width),
            vmem(block_count, width), vmem(nb2, width), vmem(nb2, width), vmem(nb4, width),
            vmem(row_count, nb4, width),
            vmem(nb4, width), vmem(nb4, width), vmem(block_count, width),
            pltpu.SMEM((row_count, cap, row_count), jnp.int32),
            pltpu.SMEM((row_count, row_count), jnp.int32),
            pltpu.SMEM((2, pairs), jnp.int32),
            dma((3,)), dma, dma((LOADS,)), dma((5,)), dma((5,)), dma, dma,
            dma, dma((row_count,)), dma, dma((row_half * CHUNKS,)),
            dma, dma((CHUNKS,)), dma, dma((2 * CHUNKS,)), dma, dma((CHUNKS,)),
        ],
        compiler_params=pltpu.CompilerParams(
            collective_id=0, has_side_effects=True, vmem_limit_bytes=60000000
        ),
        name="gram_tiles",
    )(pair_list.transpose(0, 2, 1), pair_count, pair_blocks.T, sample_rows[0], matrix)


def solution(mesh):
    in_specs = (P(("rows", "grp"), None), P(("rows", "grp"), None, None), P(), P(), P())
    out_specs = P(("rows", "grp"), None, None)
    return jax.shard_map(shards, mesh=mesh, in_specs=in_specs, out_specs=out_specs, check_vma=False)
```

```python
import functools

import jax
import jax.numpy as jnp
from jax import lax
from jax.experimental import pallas as pl
from jax.experimental.pallas import tpu as pltpu
from jax.sharding import PartitionSpec as P

epsilon = 1e-06
MESH = pl.DeviceIdType.MESH
F32 = jnp.float32
BF16 = jnp.bfloat16
SHARES = (2, 2, 2, 2)
CHUNKS = len(SHARES)
LOADS = 8
EARLY = 8
FIRST_SQUARES = 2
scope = jax.named_scope


def kernel(
    dims, list_hbm, count_hbm, blocks_hbm, samples_hbm, matrix, out, *scratch,
):
    row_count, grp_count, cap, pairs, block_count, width = dims
    it = iter(scratch)
    mat, samples, counts, places, tiles, core_in, high_in, first_in = [next(it) for _ in range(8)]
    row_in, part_b, in_b, held, part_c, in_c = [[next(it) for _ in range(CHUNKS)] for _ in range(6)]
    place_rows, scale, squares, sq_parts, sq_rows, sq_total = [next(it) for _ in range(6)]
    pair_list, pair_count, pair_blocks = [next(it) for _ in range(3)]
    (table_sem, sample_sem, place_sem, load_sem, sq_send, sq_recv, near_send, near_recv, core_send, core_recv,
     first_send, high_send, high_recv, row_send, row_recv, b_send, b_recv, c_send, c_recv) = it

    batch = block_count // LOADS
    rows_dev = mat.shape[1]
    sample_count = samples.shape[1]
    half = cap // 2
    region = pairs // row_count
    tile_dev = region // grp_count
    row_half = row_count // 2
    tall = width // 2
    sizes = [share * tall // sum(SHARES) for share in SHARES]
    starts = [sum(sizes[:q]) for q in range(CHUNKS)]
    last = row_count - 1

    s = lax.axis_index("rows")
    g = lax.axis_index("grp")
    low = lax.rem(g, 2)
    high = lax.div(g, 2)
    partner = high * 2 + (1 - low)
    across = (1 - high) * 2 + low
    corner = (1 - high) * 2 + (1 - low)
    top = lax.div(s, row_half)

    def send(source, target, send_sem, recv_sem, row, grp):
        return pltpu.make_async_remote_copy(
            src_ref=source, dst_ref=target, send_sem=send_sem, recv_sem=recv_sem,
            device_id={"rows": row, "grp": grp}, device_id_type=MESH,
        )

    def await_bytes(ref, sem):
        pltpu.make_async_copy(ref, ref, sem).wait()

    def lines_from(start, size):
        return pl.ds(pl.multiple_of(start, 8), size)

    with scope("greet"):
        barrier = pltpu.get_barrier_semaphore()

        def greet(row, grp):
            pl.semaphore_signal(barrier, inc=1, device_id={"rows": row, "grp": grp}, device_id_type=MESH)

        def greet_row(j, carry):
            greet(lax.rem(s + j, row_count), g)
            return carry

        greet(s, partner)
        greet(s, across)
        greet(s, corner)
        for j in range(1, grp_count):
            greet(s + 1 - 2 * lax.rem(s, 2), lax.rem(g + j, grp_count))
        lax.fori_loop(1, row_count, greet_row, 0)

    with scope("issue"):
        tables = [
            pltpu.make_async_copy(source, target, table_sem.at[n])
            for n, (source, target) in enumerate(
                ((list_hbm, pair_list), (count_hbm, pair_count), (blocks_hbm, pair_blocks))
            )
        ]
        sample_load = pltpu.make_async_copy(samples_hbm, samples, sample_sem)
        sample_load.start()
        for table in tables:
            table.start()
        wide = batch * width
        for i in range(LOADS):
            pltpu.make_async_copy(matrix.at[:, pl.ds(i * wide, wide)], mat.at[i], load_sem.at[i]).start(priority=1)

    def owner_of(k):
        other = 1 - lax.div(k, row_half)
        j = k + 1 - other
        return (top * (1 - other) + (1 - top) * other) * row_half + lax.rem(s + j, row_half)

    place_copy = pltpu.make_async_copy(place_rows, places, place_sem)

    def fill_places():
        pair = s * region + lax.broadcasted_iota(jnp.int32, (1, place_rows.shape[1]), 1)
        for k in range(row_count):
            source = source_of(k)
            slot = jnp.full(pair.shape, cap, jnp.int32)
            for n in range(half if k < row_half else cap):
                at = high * half + n if k < row_half else n
                slot = jnp.where(pair == pair_list[source, at, s], at, slot)
            place_rows[k : k + 1, :] = slot
        place_copy.start()

    def source_of(k):
        return ((1 - top) if k < row_half else top) * row_half + lax.rem(s + k, row_half)

    def clear(j, carry):
        for q in range(CHUNKS):
            row_in[q][j, cap] = jnp.zeros((sizes[q], width), F32)
        return carry

    lax.fori_loop(0, row_count, clear, 0)

    with scope("w_samples"):
        sample_load.wait()
        for table in tables:
            table.wait()

    early = counts.shape[0]
    part = 128
    positions = lax.broadcasted_iota(jnp.int32, (rows_dev, part), 0)
    ones = jnp.ones((part, width), BF16)

    def count_owner(i, carry):
        owner = owner_of(i)
        for n in range(cap):
            first = pair_blocks[0, pair_list[s, n, owner]]
            active = (n < pair_count[s, owner]).astype(jnp.int32)
            picked = ((samples[first] + 1) * active - 1).reshape(1, sample_count)
            hits = None
            for c in range(sample_count // part):
                hit = jnp.where(positions == picked[:, c * part : (c + 1) * part], 1.0, 0.0)
                hits = hit if hits is None else hits + hit
            multiplicity = jnp.dot(hits.astype(BF16), ones, preferred_element_type=F32)
            counts[lax.rem(i, early), n] = multiplicity.astype(BF16)
        return carry

    with scope("places"):
        fill_places()
    with scope("counts"):
        lax.fori_loop(0, early, count_owner, 0)

    def square_batch(i, carry):
        for u in range(batch // 8):
            lines = []
            for m in range(8):
                values = mat[i, :, (u * 8 + m) * width : (u * 8 + m + 1) * width].astype(F32)
                lines.append(jnp.sum(values * values, axis=0, keepdims=True))
            squares[lines_from(i * batch + u * 8, 8), :] = jnp.concatenate(lines, axis=0)
        return carry

    def load_batch(i, carry):
        with scope("w_load"):
            await_bytes(mat.at[i], load_sem.at[i])
        return square_batch(i, carry)

    def load_wait(i, carry):
        await_bytes(mat.at[i], load_sem.at[i])
        return carry

    with scope("load_sq"):
        lax.fori_loop(0, FIRST_SQUARES, load_batch, 0)
    with scope("load_rest"):
        lax.fori_loop(FIRST_SQUARES, LOADS, load_wait, 0)

    nb8 = block_count // 8
    side = lax.rem(s, 2)
    seat = side * grp_count + g
    peers = [lax.rem(seat + j, 8) for j in range(1, 8)]

    def eighth(peer):
        grp = lax.rem(peer, grp_count)
        at = lax.rem(grp, 2) * 4 + lax.div(grp, 2) * 2 + lax.div(peer, grp_count)
        return lines_from(at * nb8, nb8)

    def peer_row(peer):
        return s - side + lax.div(peer, grp_count)

    def sq_first():
        for peer in peers:
            send(
                squares.at[eighth(peer)], sq_parts.at[seat], sq_send.at[0], sq_recv.at[0],
                peer_row(peer), lax.rem(peer, grp_count),
            ).start()

    def even_row(j):
        return lax.rem(s + 2 * j, row_count)

    def sq_second():
        await_bytes(sq_parts.at[pl.ds(0, 7)], sq_recv.at[0])
        total = squares[eighth(seat), :]
        for peer in peers:
            total = total + sq_parts[peer]
        sq_rows[s] = total

        def sq_row(j, carry):
            send(sq_rows.at[s], sq_rows.at[s], near_send, near_recv, even_row(j), g).start()
            return carry

        lax.fori_loop(1, row_half, sq_row, 0)

    def sq_third():
        await_bytes(sq_rows.at[pl.ds(0, row_half - 1)], near_recv)
        total = sq_rows[s]
        for j in range(1, row_half):
            total = total + sq_rows[even_row(j)]
        here = eighth(seat)
        sq_total[here, :] = total
        for peer in peers:
            send(
                sq_total.at[here], sq_total.at[here], sq_send.at[1], sq_recv.at[1],
                peer_row(peer), lax.rem(peer, grp_count),
            ).start()

    my_lines = lines_from(low * tall, tall)
    their_lines = lines_from((1 - low) * tall, tall)
    mine = pl.ds(high * half, half)
    theirs = pl.ds((1 - high) * half, half)
    every = pl.ds(0, cap)

    def lines(q):
        return lines_from(low * tall + starts[q], sizes[q])

    def within(q):
        return pl.ds(starts[q] - sizes[0], sizes[q])

    def core_copy(k):
        return send(tiles.at[k, every, their_lines], core_in.at[k], core_send, core_recv.at[k], s, partner)

    def high_copy(k, q):
        target = high_in.at[k, pl.ds(0, half), within(q)]
        arrived = high_recv.at[row_half + q - 1]
        return send(tiles.at[k, theirs, lines(q)], target, high_send, arrived, s, across)

    def first_copy(k, t):
        there = lines(0) if t == 0 else lines_from((1 - low) * tall, sizes[0])
        target = first_in.at[k, t]
        return send(tiles.at[k, theirs, there], target, first_send, high_recv.at[k], s, across if t == 0 else corner)

    def far_copy(k, q):
        return send(tiles.at[k, mine, lines(q)], row_in[q].at[s, mine], row_send, row_recv.at[q], owner_of(k), g)

    def near_copy(k, q):
        return send(tiles.at[k, every, lines(q)], row_in[q].at[s, every], row_send, row_recv.at[q], owner_of(k), g)

    def block(b):
        return mat[lax.div(b, batch), :, pl.ds(lax.rem(b, batch) * width, width)]

    def make(k):
        owner = owner_of(k)
        for n in range(cap):
            pair = pair_list[s, n, owner]
            weighted = counts[lax.rem(k, early), n] * block(pair_blocks[0, pair])
            tiles[k, n] = lax.dot_general(
                weighted, block(pair_blocks[1, pair]), (((0,), (0,)), ((), ())),
                preferred_element_type=F32,
            )

    later = lines_from(low * tall + sizes[0], tall - sizes[0])

    def fold_far(k):
        core_copy(k).wait_recv()
        tiles[k, :, later] = tiles[k, :, later] + core_in[k, :, sizes[0] :]
        high_copy(k, 1).start()

    def fold_near(k):
        core_copy(k).wait_recv()
        tiles[k, :, my_lines] = tiles[k, :, my_lines] + core_in[k]

    def cross_first(k):
        await_bytes(first_in.at[k], high_recv.at[k])
        own = tiles[k, mine, lines(0)] + core_in[k, mine, 0 : sizes[0]]
        tiles[k, mine, lines(0)] = own + (first_in[k, 0] + first_in[k, 1])
        far_copy(k, 0).start()

    def cross(k, q):
        tiles[k, mine, lines(q)] = tiles[k, mine, lines(q)] + high_in[k, :, within(q)]
        far_copy(k, q).start()

    def produce(k):
        if early < row_count:
            @pl.when(k >= early)
            def _():
                with scope("count"):
                    count_owner(k, 0)

        with scope("make"):
            make(k)

    def deliver(k):
        core_copy(k).start()
        for t in range(2):
            first_copy(k, t).start()

    def high_go(q):
        def go(k, carry):
            high_copy(k, q).start()
            return carry

        lax.fori_loop(0, row_half, go, 0)

    produce(0)
    with scope("barrier"):
        pl.semaphore_wait(barrier, row_count + 5)
    deliver(0)

    def far_step(k, carry):
        produce(k)
        deliver(k)
        return carry

    def near_step(j, carry):
        produce(row_half + j)
        core_copy(row_half + j).start()
        with scope("fold"):
            fold_far(j)
        return carry

    def sum_step(j, carry):
        with scope("cross0"):
            cross_first(j)
        with scope("fold"):
            fold_near(row_half + j)

        @pl.when(row_half + j < last)
        def _():
            near_copy(row_half + j, 0).start()

        @pl.when(FIRST_SQUARES + j < LOADS)
        def _():
            with scope("squares"):
                square_batch(FIRST_SQUARES + j, 0)

        return carry

    lax.fori_loop(1, row_half, far_step, 0)
    lax.fori_loop(0, row_half, near_step, 0)
    high_go(2)
    lax.fori_loop(0, row_half, sum_step, 0)
    with scope("squares"):
        lax.fori_loop(min(FIRST_SQUARES + row_half, LOADS), LOADS, square_batch, 0)
    sq_first()
    for q in range(3, CHUNKS):
        high_go(q)

    def crosses(q):
        def near_go(k, carry):
            near_copy(k, q).start()
            return carry

        def cross_go(k, carry):
            cross(k, q)
            return carry

        with scope("crosses"):
            lax.fori_loop(row_half, last, near_go, 0)
            await_bytes(high_in.at[:, :, within(q)], high_recv.at[row_half + q - 1])
            lax.fori_loop(0, row_half, cross_go, 0)

    crosses(1)
    crosses(2)
    with scope("sq_second"):
        sq_second()
    for q in range(CHUNKS):
        row_in[q][s, every] = tiles[last, :, lines(q)]

    def owned(q, grp, n):
        j = grp * tile_dev + n
        total = row_in[q][source_of(0), places[0, j]]
        for k in range(1, row_count):
            total = total + row_in[q][source_of(k), places[k, j]]
        return total

    distant = ((1 - high) * 2 + (1 - low), (1 - high) * 2 + low)
    local = (partner, g)

    def b_copy(q, t):
        return send(part_b[q].at[t], in_b[q].at[t], b_send, b_recv.at[q * 2 + t], s, across)

    def c_copy(q):
        return send(part_c[q], in_c[q], c_send, c_recv.at[q], s, partner)

    arriving = 3 * row_count // 4 - 1

    def post(q):
        with scope("w_rows"):
            await_bytes(row_in[q].at[pl.ds(0, arriving), every], row_recv.at[q])
        with scope("post"):
            for t in range(2):
                def away(n, carry):
                    part_b[q][t, n] = owned(q, distant[t], n)
                    return carry

                lax.fori_loop(0, tile_dev, away, 0)
                b_copy(q, t).start()
            for t in range(2):
                def hold(n, carry):
                    held[q][t, n] = owned(q, local[t], n)
                    return carry

                lax.fori_loop(0, tile_dev, hold, 0)

    def store(place, values, scaled):
        out[:, place] = values * scale[:, place] if scaled else values

    def finish(q, scaled=False):
        with scope("w_b0"):
            b_copy(q, 0).wait_recv()
        part_c[q][...] = held[q][0] + in_b[q][0]
        c_copy(q).start()
        with scope("w_b1"):
            b_copy(q, 1).wait_recv()
        store(lines(q), held[q][1] + in_b[q][1], scaled)

    def collect(q, scaled=False):
        with scope("w_c"):
            c_copy(q).wait_recv()
        store(lines_from((1 - low) * tall + starts[q], sizes[q]), in_c[q][...], scaled)

    def factors():
        await_bytes(sq_total.at[pl.ds(0, 7 * nb8)], sq_recv.at[1])
        await_bytes(sq_parts.at[pl.ds(0, 7)], sq_send.at[1])
        sq_total[...] = jnp.sqrt(sq_total[...] / (rows_dev * row_count * grp_count) + epsilon)

        def factor(n, carry):
            pair = (s * region + g * tile_dev) + n
            left = sq_total[pair_blocks[0, pair]].reshape(1, width)
            right = sq_total[pair_blocks[1, pair]].reshape(1, width)
            left = jnp.broadcast_to(left, (width, width)).T
            scale[n] = 1.0 / (sample_count * left * right)
            return carry

        lax.fori_loop(0, tile_dev, factor, 0)

    def rescale(start, size):
        piece = lines_from(start, size)
        out[:, piece] = out[:, piece] * scale[:, piece]

    with scope("w_places"):
        place_copy.wait()
    post(0)
    crosses(3)
    post(1)
    finish(0)
    post(2)
    with scope("sq_third"):
        sq_third()
    finish(1)
    collect(0)
    post(3)
    finish(2)
    collect(1)
    with scope("factors"):
        factors()
    rescale(low * tall, starts[CHUNKS - 1])
    rescale((1 - low) * tall, starts[CHUNKS - 2])
    finish(CHUNKS - 1, True)
    collect(CHUNKS - 2, True)
    collect(CHUNKS - 1, True)

    with scope("drain"):
        await_bytes(core_in, core_send)
        await_bytes(first_in, first_send)
        await_bytes(high_in, high_send)
        await_bytes(tiles.at[pl.ds(0, arriving), every, pl.ds(0, tall)], row_send)
        await_bytes(tiles.at[pl.ds(0, tile_dev // cap), every, pl.ds(0, tall)], c_send)
        await_bytes(tiles.at[pl.ds(0, 2 * tile_dev // cap), every, pl.ds(0, tall)], b_send)
        await_bytes(sq_rows.at[pl.ds(0, row_half - 1)], near_send)
        await_bytes(sq_parts.at[pl.ds(0, 7)], sq_send.at[0])


def shards(matrix, sample_rows, pair_list, pair_count, pair_blocks):
    rows_dev, column_count = matrix.shape
    block_count, sample_count = sample_rows.shape[1:]
    width = column_count // block_count
    row_count = lax.axis_size("rows")
    grp_count = lax.axis_size("grp")
    cap = pair_list.shape[2]
    pairs = pair_blocks.shape[0]
    region = pairs // row_count
    tile_dev = region // grp_count
    half = cap // 2
    row_half = row_count // 2
    tall = width // 2
    sizes = [share * tall // sum(SHARES) for share in SHARES]
    nb8 = block_count // 8
    early = min(row_count, EARLY)
    dma = pltpu.SemaphoreType.DMA

    def vmem(*shape):
        return pltpu.VMEM(shape, F32)

    def smem(*shape):
        return pltpu.SMEM(shape, jnp.int32)

    dims = (row_count, grp_count, cap, pairs, block_count, width)
    return pl.pallas_call(
        functools.partial(kernel, dims),
        out_shape=pltpu.VMEM((tile_dev, width, width), F32),
        in_specs=[pl.BlockSpec(memory_space=pl.ANY) for _ in range(5)],
        out_specs=pl.BlockSpec(memory_space=pltpu.VMEM),
        scratch_shapes=[
            pltpu.VMEM((LOADS, rows_dev, column_count // LOADS), BF16),
            pltpu.VMEM((block_count, sample_count), jnp.int32),
            pltpu.VMEM((early, cap, rows_dev, width), BF16),
            smem(row_count, 128),
            vmem(row_count, cap, width, width),
            vmem(row_count, cap, tall, width),
            vmem(row_half, half, tall - sizes[0], width),
            vmem(row_half, 2, half, sizes[0], width),
            *[vmem(row_count, cap + 1, size, width) for size in sizes],
            *[vmem(2, tile_dev, size, width) for size in sizes],
            *[vmem(2, tile_dev, size, width) for size in sizes],
            *[vmem(2, tile_dev, size, width) for size in sizes],
            *[vmem(tile_dev, size, width) for size in sizes],
            *[vmem(tile_dev, size, width) for size in sizes],
            pltpu.VMEM((row_count, 128), jnp.int32),
            vmem(tile_dev, width, width),
            vmem(block_count, width), vmem(8, nb8, width), vmem(row_count, nb8, width),
            vmem(block_count, width),
            smem(row_count, cap, row_count), smem(row_count, row_count), smem(2, pairs),
            dma((3,)), dma, dma, dma((LOADS,)), dma((2,)), dma((2,)), dma, dma, dma, dma((row_count,)),
            dma, dma, dma((row_half + CHUNKS - 1,)), dma, dma((CHUNKS,)),
            dma, dma((2 * CHUNKS,)), dma, dma((CHUNKS,)),
        ],
        compiler_params=pltpu.CompilerParams(
            collective_id=0, has_side_effects=True, vmem_limit_bytes=60000000
        ),
        name="gram_tiles",
    )(pair_list.transpose(0, 2, 1), pair_count, pair_blocks.T, sample_rows[0], matrix)


def solution(mesh):
    in_specs = (P(("rows", "grp"), None), P(("rows", "grp"), None, None), P(), P(), P())
    out_specs = P(("rows", "grp"), None, None)
    return jax.shard_map(shards, mesh=mesh, in_specs=in_specs, out_specs=out_specs, check_vma=False)
```

```python
import functools

import jax
import jax.numpy as jnp
from jax import lax
from jax.experimental import pallas as pl
from jax.experimental.pallas import tpu as pltpu
from jax.sharding import PartitionSpec as P

epsilon = 1e-06
MESH = pl.DeviceIdType.MESH
F32 = jnp.float32
BF16 = jnp.bfloat16
SHARES = (2, 2, 2, 2)
CHUNKS = len(SHARES)
LOADS = 8
EARLY = 8
FIRST_SQUARES = 2
scope = jax.named_scope


def kernel(
    dims, list_hbm, count_hbm, blocks_hbm, samples_hbm, matrix, out, *scratch,
):
    row_count, grp_count, cap, pairs, block_count, width = dims
    it = iter(scratch)
    mat, samples, counts, places, tiles, core_in, high_in, first_in = [next(it) for _ in range(8)]
    row_in, part_b, in_b, held, part_c, in_c = [[next(it) for _ in range(CHUNKS)] for _ in range(6)]
    place_rows, scale, squares, sq_parts, sq_rows, sq_total = [next(it) for _ in range(6)]
    pair_list, pair_count, pair_blocks = [next(it) for _ in range(3)]
    (table_sem, sample_sem, place_sem, load_sem, sq_send, sq_recv, near_send, near_recv, core_send, core_recv,
     first_send, high_send, high_recv, row_send, row_recv, b_send, b_recv, c_send, c_recv) = it

    batch = block_count // LOADS
    rows_dev = mat.shape[1]
    sample_count = samples.shape[1]
    half = cap // 2
    region = pairs // row_count
    tile_dev = region // grp_count
    row_half = row_count // 2
    tall = width // 2
    sizes = [share * tall // sum(SHARES) for share in SHARES]
    starts = [sum(sizes[:q]) for q in range(CHUNKS)]
    last = row_count - 1

    s = lax.axis_index("rows")
    g = lax.axis_index("grp")
    low = lax.rem(g, 2)
    high = lax.div(g, 2)
    partner = high * 2 + (1 - low)
    across = (1 - high) * 2 + low
    corner = (1 - high) * 2 + (1 - low)
    top = lax.div(s, row_half)

    def send(source, target, send_sem, recv_sem, row, grp):
        return pltpu.make_async_remote_copy(
            src_ref=source, dst_ref=target, send_sem=send_sem, recv_sem=recv_sem,
            device_id={"rows": row, "grp": grp}, device_id_type=MESH,
        )

    def await_bytes(ref, sem):
        pltpu.make_async_copy(ref, ref, sem).wait()

    def lines_from(start, size):
        return pl.ds(pl.multiple_of(start, 8), size)

    with scope("greet"):
        barrier = pltpu.get_barrier_semaphore()

        def greet(row, grp):
            pl.semaphore_signal(barrier, inc=1, device_id={"rows": row, "grp": grp}, device_id_type=MESH)

        def greet_row(j, carry):
            greet(lax.rem(s + j, row_count), g)
            return carry

        greet(s, partner)
        greet(s, across)
        greet(s, corner)
        for j in range(1, grp_count):
            greet(s + 1 - 2 * lax.rem(s, 2), lax.rem(g + j, grp_count))
        lax.fori_loop(1, row_count, greet_row, 0)

    with scope("issue"):
        tables = [
            pltpu.make_async_copy(source, target, table_sem.at[n])
            for n, (source, target) in enumerate(
                ((list_hbm, pair_list), (count_hbm, pair_count), (blocks_hbm, pair_blocks))
            )
        ]
        sample_load = pltpu.make_async_copy(samples_hbm, samples, sample_sem)
        sample_load.start()
        for table in tables:
            table.start()
        wide = batch * width
        for i in range(LOADS):
            pltpu.make_async_copy(matrix.at[:, pl.ds(i * wide, wide)], mat.at[i], load_sem.at[i]).start(priority=1)

    def owner_of(k):
        other = 1 - lax.div(k, row_half)
        j = k + 1 - other
        return (top * (1 - other) + (1 - top) * other) * row_half + lax.rem(s + j, row_half)

    place_copy = pltpu.make_async_copy(place_rows, places, place_sem)

    def fill_places():
        pair = s * region + lax.broadcasted_iota(jnp.int32, (1, place_rows.shape[1]), 1)
        for k in range(row_count):
            source = source_of(k)
            slot = jnp.full(pair.shape, cap, jnp.int32)
            for n in range(half if k < row_half else cap):
                at = high * half + n if k < row_half else n
                slot = jnp.where(pair == pair_list[source, at, s], at, slot)
            place_rows[k : k + 1, :] = slot
        place_copy.start()

    def source_of(k):
        return ((1 - top) if k < row_half else top) * row_half + lax.rem(s + k, row_half)

    def clear(j, carry):
        for q in range(CHUNKS):
            row_in[q][j, cap] = jnp.zeros((sizes[q], width), F32)
        return carry

    lax.fori_loop(0, row_count, clear, 0)

    with scope("w_samples"):
        sample_load.wait()
        for table in tables:
            table.wait()

    early = counts.shape[0]
    part = 128
    positions = lax.broadcasted_iota(jnp.int32, (rows_dev, part), 0)
    ones = jnp.ones((part, width), BF16)

    def count_owner(i, carry):
        owner = owner_of(i)
        for n in range(cap):
            first = pair_blocks[0, pair_list[s, n, owner]]
            active = (n < pair_count[s, owner]).astype(jnp.int32)
            picked = ((samples[first] + 1) * active - 1).reshape(1, sample_count)
            hits = None
            for c in range(sample_count // part):
                hit = jnp.where(positions == picked[:, c * part : (c + 1) * part], 1.0, 0.0)
                hits = hit if hits is None else hits + hit
            multiplicity = jnp.dot(hits.astype(BF16), ones, preferred_element_type=F32)
            counts[lax.rem(i, early), n] = multiplicity.astype(BF16)
        return carry

    with scope("places"):
        fill_places()
    with scope("counts"):
        lax.fori_loop(0, early, count_owner, 0)

    def square_batch(i, carry):
        for u in range(batch // 8):
            lines = []
            for m in range(8):
                values = mat[i, :, (u * 8 + m) * width : (u * 8 + m + 1) * width].astype(F32)
                lines.append(jnp.sum(values * values, axis=0, keepdims=True))
            squares[lines_from(i * batch + u * 8, 8), :] = jnp.concatenate(lines, axis=0)
        return carry

    def load_batch(i, carry):
        with scope("w_load"):
            await_bytes(mat.at[i], load_sem.at[i])
        return square_batch(i, carry)

    def load_wait(i, carry):
        await_bytes(mat.at[i], load_sem.at[i])
        return carry

    with scope("load_sq"):
        lax.fori_loop(0, FIRST_SQUARES, load_batch, 0)
    with scope("load_rest"):
        lax.fori_loop(FIRST_SQUARES, LOADS, load_wait, 0)

    nb8 = block_count // 8
    side = lax.rem(s, 2)
    seat = side * grp_count + g
    peers = [lax.rem(seat + j, 8) for j in range(1, 8)]

    def eighth(peer):
        grp = lax.rem(peer, grp_count)
        at = lax.rem(grp, 2) * 4 + lax.div(grp, 2) * 2 + lax.div(peer, grp_count)
        return lines_from(at * nb8, nb8)

    def peer_row(peer):
        return s - side + lax.div(peer, grp_count)

    def sq_first():
        for peer in peers:
            send(
                squares.at[eighth(peer)], sq_parts.at[seat], sq_send.at[0], sq_recv.at[0],
                peer_row(peer), lax.rem(peer, grp_count),
            ).start()

    def even_row(j):
        return lax.rem(s + 2 * j, row_count)

    def sq_second():
        await_bytes(sq_parts.at[pl.ds(0, 7)], sq_recv.at[0])
        total = squares[eighth(seat), :]
        for peer in peers:
            total = total + sq_parts[peer]
        sq_rows[s] = total

        def sq_row(j, carry):
            send(sq_rows.at[s], sq_rows.at[s], near_send, near_recv, even_row(j), g).start()
            return carry

        lax.fori_loop(1, row_half, sq_row, 0)

    def sq_third():
        await_bytes(sq_rows.at[pl.ds(0, row_half - 1)], near_recv)
        total = sq_rows[s]
        for j in range(1, row_half):
            total = total + sq_rows[even_row(j)]
        here = eighth(seat)
        sq_total[here, :] = total
        for peer in peers:
            send(
                sq_total.at[here], sq_total.at[here], sq_send.at[1], sq_recv.at[1],
                peer_row(peer), lax.rem(peer, grp_count),
            ).start()

    my_lines = lines_from(low * tall, tall)
    their_lines = lines_from((1 - low) * tall, tall)
    mine = pl.ds(high * half, half)
    theirs = pl.ds((1 - high) * half, half)
    every = pl.ds(0, cap)

    def lines(q):
        return lines_from(low * tall + starts[q], sizes[q])

    def within(q):
        return pl.ds(starts[q] - sizes[0], sizes[q])

    def core_copy(k):
        return send(tiles.at[k, every, their_lines], core_in.at[k], core_send, core_recv.at[k], s, partner)

    def high_copy(k, q):
        target = high_in.at[k, pl.ds(0, half), within(q)]
        arrived = high_recv.at[row_half + q - 1]
        return send(tiles.at[k, theirs, lines(q)], target, high_send, arrived, s, across)

    def first_copy(k, t):
        there = lines(0) if t == 0 else lines_from((1 - low) * tall, sizes[0])
        target = first_in.at[k, t]
        return send(tiles.at[k, theirs, there], target, first_send, high_recv.at[k], s, across if t == 0 else corner)

    def far_copy(k, q):
        return send(tiles.at[k, mine, lines(q)], row_in[q].at[s, mine], row_send, row_recv.at[q], owner_of(k), g)

    def near_copy(k, q):
        return send(tiles.at[k, every, lines(q)], row_in[q].at[s, every], row_send, row_recv.at[q], owner_of(k), g)

    def block(b):
        return mat[lax.div(b, batch), :, pl.ds(lax.rem(b, batch) * width, width)]

    def make(k):
        owner = owner_of(k)
        for n in range(cap):
            pair = pair_list[s, n, owner]
            weighted = counts[lax.rem(k, early), n] * block(pair_blocks[0, pair])
            tiles[k, n] = lax.dot_general(
                weighted, block(pair_blocks[1, pair]), (((0,), (0,)), ((), ())),
                preferred_element_type=F32,
            )

    later = lines_from(low * tall + sizes[0], tall - sizes[0])

    def fold_far(k):
        core_copy(k).wait_recv()
        tiles[k, :, later] = tiles[k, :, later] + core_in[k, :, sizes[0] :]
        high_copy(k, 1).start()

    def fold_near(k):
        core_copy(k).wait_recv()
        tiles[k, :, my_lines] = tiles[k, :, my_lines] + core_in[k]

    def cross_first(k):
        await_bytes(first_in.at[k], high_recv.at[k])
        own = tiles[k, mine, lines(0)] + core_in[k, mine, 0 : sizes[0]]
        tiles[k, mine, lines(0)] = own + (first_in[k, 0] + first_in[k, 1])
        far_copy(k, 0).start()

    def cross(k, q):
        tiles[k, mine, lines(q)] = tiles[k, mine, lines(q)] + high_in[k, :, within(q)]
        far_copy(k, q).start()

    def produce(k):
        if early < row_count:
            @pl.when(k >= early)
            def _():
                with scope("count"):
                    count_owner(k, 0)

        with scope("make"):
            make(k)

    def deliver(k):
        core_copy(k).start()
        for t in range(2):
            first_copy(k, t).start()

    def high_go(q):
        def go(k, carry):
            high_copy(k, q).start()
            return carry

        lax.fori_loop(0, row_half, go, 0)

    produce(0)
    with scope("barrier"):
        pl.semaphore_wait(barrier, row_count + 5)
    deliver(0)

    def far_step(k, carry):
        produce(k)
        deliver(k)
        return carry

    def near_step(j, carry):
        produce(row_half + j)
        core_copy(row_half + j).start()
        with scope("fold"):
            fold_far(j)
        return carry

    def sum_step(j, carry):
        with scope("cross0"):
            cross_first(j)
        with scope("fold"):
            fold_near(row_half + j)

        @pl.when(row_half + j < last)
        def _():
            near_copy(row_half + j, 0).start()

        @pl.when(FIRST_SQUARES + j < LOADS)
        def _():
            with scope("squares"):
                square_batch(FIRST_SQUARES + j, 0)

        return carry

    lax.fori_loop(1, row_half, far_step, 0)
    lax.fori_loop(0, row_half, near_step, 0)
    @pl.when(low == 0)
    def _():
        high_go(2)

    lax.fori_loop(0, row_half, sum_step, 0)

    @pl.when(low == 1)
    def _():
        high_go(2)

    with scope("squares"):
        lax.fori_loop(min(FIRST_SQUARES + row_half, LOADS), LOADS, square_batch, 0)
    sq_first()
    for q in range(3, CHUNKS):
        high_go(q)

    def crosses(q):
        def near_go(k, carry):
            near_copy(k, q).start()
            return carry

        def cross_go(k, carry):
            cross(k, q)
            return carry

        with scope("crosses"):
            @pl.when(low == 0)
            def _():
                lax.fori_loop(row_half, last, near_go, 0)

            await_bytes(high_in.at[:, :, within(q)], high_recv.at[row_half + q - 1])
            lax.fori_loop(0, row_half, cross_go, 0)

            @pl.when(low == 1)
            def _():
                lax.fori_loop(row_half, last, near_go, 0)

    crosses(1)
    crosses(2)
    for q in range(CHUNKS):
        row_in[q][s, every] = tiles[last, :, lines(q)]

    def owned(q, grp, n):
        j = grp * tile_dev + n
        total = row_in[q][source_of(0), places[0, j]]
        for k in range(1, row_count):
            total = total + row_in[q][source_of(k), places[k, j]]
        return total

    distant = ((1 - high) * 2 + (1 - low), (1 - high) * 2 + low)
    local = (partner, g)

    def b_copy(q, t):
        return send(part_b[q].at[t], in_b[q].at[t], b_send, b_recv.at[q * 2 + t], s, across)

    def c_copy(q):
        return send(part_c[q], in_c[q], c_send, c_recv.at[q], s, partner)

    arriving = 3 * row_count // 4 - 1

    def post(q):
        with scope("w_rows"):
            await_bytes(row_in[q].at[pl.ds(0, arriving), every], row_recv.at[q])
        with scope("post"):
            for t in range(2):
                def away(n, carry):
                    part_b[q][t, n] = owned(q, distant[t], n)
                    return carry

                lax.fori_loop(0, tile_dev, away, 0)
                b_copy(q, t).start()
            for t in range(2):
                def hold(n, carry):
                    held[q][t, n] = owned(q, local[t], n)
                    return carry

                lax.fori_loop(0, tile_dev, hold, 0)

    def store(place, values, scaled):
        out[:, place] = values * scale[:, place] if scaled else values

    def finish(q, scaled=False):
        with scope("w_b0"):
            b_copy(q, 0).wait_recv()
        part_c[q][...] = held[q][0] + in_b[q][0]
        c_copy(q).start()
        with scope("w_b1"):
            b_copy(q, 1).wait_recv()
        store(lines(q), held[q][1] + in_b[q][1], scaled)

    def collect(q, scaled=False):
        with scope("w_c"):
            c_copy(q).wait_recv()
        store(lines_from((1 - low) * tall + starts[q], sizes[q]), in_c[q][...], scaled)

    def factors():
        await_bytes(sq_total.at[pl.ds(0, 7 * nb8)], sq_recv.at[1])
        await_bytes(sq_parts.at[pl.ds(0, 7)], sq_send.at[1])
        sq_total[...] = jnp.sqrt(sq_total[...] / (rows_dev * row_count * grp_count) + epsilon)

        def factor(n, carry):
            pair = (s * region + g * tile_dev) + n
            left = sq_total[pair_blocks[0, pair]].reshape(1, width)
            right = sq_total[pair_blocks[1, pair]].reshape(1, width)
            left = jnp.broadcast_to(left, (width, width)).T
            scale[n] = 1.0 / (sample_count * left * right)
            return carry

        lax.fori_loop(0, tile_dev, factor, 0)

    def rescale(start, size):
        piece = lines_from(start, size)
        out[:, piece] = out[:, piece] * scale[:, piece]

    with scope("w_places"):
        place_copy.wait()
    post(0)
    with scope("sq_second"):
        sq_second()
    for q in range(3, CHUNKS):
        crosses(q)
    post(1)
    finish(0)
    post(2)
    with scope("sq_third"):
        sq_third()
    finish(1)
    collect(0)
    for q in range(3, CHUNKS):
        post(q)
        finish(q - 1)
        collect(q - 2)
    with scope("factors"):
        factors()
    rescale(low * tall, starts[CHUNKS - 1])
    rescale((1 - low) * tall, starts[CHUNKS - 2])
    finish(CHUNKS - 1, True)
    collect(CHUNKS - 2, True)
    collect(CHUNKS - 1, True)

    with scope("drain"):
        await_bytes(core_in, core_send)
        await_bytes(first_in, first_send)
        await_bytes(high_in, high_send)
        await_bytes(tiles.at[pl.ds(0, arriving), every, pl.ds(0, tall)], row_send)
        await_bytes(tiles.at[pl.ds(0, tile_dev // cap), every, pl.ds(0, tall)], c_send)
        await_bytes(tiles.at[pl.ds(0, 2 * tile_dev // cap), every, pl.ds(0, tall)], b_send)
        await_bytes(sq_rows.at[pl.ds(0, row_half - 1)], near_send)
        await_bytes(sq_parts.at[pl.ds(0, 7)], sq_send.at[0])


def shards(matrix, sample_rows, pair_list, pair_count, pair_blocks):
    rows_dev, column_count = matrix.shape
    block_count, sample_count = sample_rows.shape[1:]
    width = column_count // block_count
    row_count = lax.axis_size("rows")
    grp_count = lax.axis_size("grp")
    cap = pair_list.shape[2]
    pairs = pair_blocks.shape[0]
    region = pairs // row_count
    tile_dev = region // grp_count
    half = cap // 2
    row_half = row_count // 2
    tall = width // 2
    sizes = [share * tall // sum(SHARES) for share in SHARES]
    nb8 = block_count // 8
    early = min(row_count, EARLY)
    dma = pltpu.SemaphoreType.DMA

    def vmem(*shape):
        return pltpu.VMEM(shape, F32)

    def smem(*shape):
        return pltpu.SMEM(shape, jnp.int32)

    dims = (row_count, grp_count, cap, pairs, block_count, width)
    return pl.pallas_call(
        functools.partial(kernel, dims),
        out_shape=pltpu.VMEM((tile_dev, width, width), F32),
        in_specs=[pl.BlockSpec(memory_space=pl.ANY) for _ in range(5)],
        out_specs=pl.BlockSpec(memory_space=pltpu.VMEM),
        scratch_shapes=[
            pltpu.VMEM((LOADS, rows_dev, column_count // LOADS), BF16),
            pltpu.VMEM((block_count, sample_count), jnp.int32),
            pltpu.VMEM((early, cap, rows_dev, width), BF16),
            smem(row_count, 128),
            vmem(row_count, cap, width, width),
            vmem(row_count, cap, tall, width),
            vmem(row_half, half, tall - sizes[0], width),
            vmem(row_half, 2, half, sizes[0], width),
            *[vmem(row_count, cap + 1, size, width) for size in sizes],
            *[vmem(2, tile_dev, size, width) for size in sizes],
            *[vmem(2, tile_dev, size, width) for size in sizes],
            *[vmem(2, tile_dev, size, width) for size in sizes],
            *[vmem(tile_dev, size, width) for size in sizes],
            *[vmem(tile_dev, size, width) for size in sizes],
            pltpu.VMEM((row_count, 128), jnp.int32),
            vmem(tile_dev, width, width),
            vmem(block_count, width), vmem(8, nb8, width), vmem(row_count, nb8, width),
            vmem(block_count, width),
            smem(row_count, cap, row_count), smem(row_count, row_count), smem(2, pairs),
            dma((3,)), dma, dma, dma((LOADS,)), dma((2,)), dma((2,)), dma, dma, dma, dma((row_count,)),
            dma, dma, dma((row_half + CHUNKS - 1,)), dma, dma((CHUNKS,)),
            dma, dma((2 * CHUNKS,)), dma, dma((CHUNKS,)),
        ],
        compiler_params=pltpu.CompilerParams(
            collective_id=0, has_side_effects=True, vmem_limit_bytes=60000000
        ),
        name="gram_tiles",
    )(pair_list.transpose(0, 2, 1), pair_count, pair_blocks.T, sample_rows[0], matrix)


def solution(mesh):
    in_specs = (P(("rows", "grp"), None), P(("rows", "grp"), None, None), P(), P(), P())
    out_specs = P(("rows", "grp"), None, None)
    return jax.shard_map(shards, mesh=mesh, in_specs=in_specs, out_specs=out_specs, check_vma=False)
```

```python
import functools

import jax
import jax.numpy as jnp
from jax import lax
from jax.experimental import pallas as pl
from jax.experimental.pallas import tpu as pltpu
from jax.sharding import PartitionSpec as P

epsilon = 1e-06
MESH = pl.DeviceIdType.MESH
F32 = jnp.float32
BF16 = jnp.bfloat16
SHARES = (2, 2, 2, 2)
CHUNKS = len(SHARES)
LOADS = 8
EARLY = 8
FIRST_SQUARES = 2
scope = jax.named_scope


def kernel(
    dims, list_hbm, count_hbm, blocks_hbm, samples_hbm, matrix, out, *scratch,
):
    row_count, grp_count, cap, pairs, block_count, width = dims
    it = iter(scratch)
    mat, samples, counts, places, tiles, core_in, high_in, first_in = [next(it) for _ in range(8)]
    row_in, part_b, in_b, held, part_c, in_c = [[next(it) for _ in range(CHUNKS)] for _ in range(6)]
    place_rows, scale, squares, sq_parts, sq_rows, sq_total = [next(it) for _ in range(6)]
    pair_list, pair_count, pair_blocks = [next(it) for _ in range(3)]
    (table_sem, sample_sem, load_sem, sq_send, sq_recv, near_send, near_recv, core_send, core_recv,
     first_send, high_send, high_recv, row_send, row_recv, b_send, b_recv, c_send, c_recv) = it

    batch = block_count // LOADS
    rows_dev = mat.shape[1]
    sample_count = samples.shape[1]
    half = cap // 2
    region = pairs // row_count
    tile_dev = region // grp_count
    row_half = row_count // 2
    tall = width // 2
    sizes = [share * tall // sum(SHARES) for share in SHARES]
    starts = [sum(sizes[:q]) for q in range(CHUNKS)]
    last = row_count - 1

    s = lax.axis_index("rows")
    g = lax.axis_index("grp")
    low = lax.rem(g, 2)
    high = lax.div(g, 2)
    partner = high * 2 + (1 - low)
    across = (1 - high) * 2 + low
    corner = (1 - high) * 2 + (1 - low)
    top = lax.div(s, row_half)

    def send(source, target, send_sem, recv_sem, row, grp):
        return pltpu.make_async_remote_copy(
            src_ref=source, dst_ref=target, send_sem=send_sem, recv_sem=recv_sem,
            device_id={"rows": row, "grp": grp}, device_id_type=MESH,
        )

    def await_bytes(ref, sem):
        pltpu.make_async_copy(ref, ref, sem).wait()

    def lines_from(start, size):
        return pl.ds(pl.multiple_of(start, 8), size)

    with scope("greet"):
        barrier = pltpu.get_barrier_semaphore()

        def greet(row, grp):
            pl.semaphore_signal(barrier, inc=1, device_id={"rows": row, "grp": grp}, device_id_type=MESH)

        def greet_row(j, carry):
            greet(lax.rem(s + j, row_count), g)
            return carry

        greet(s, partner)
        greet(s, across)
        greet(s, corner)
        for j in range(1, grp_count):
            greet(s + 1 - 2 * lax.rem(s, 2), lax.rem(g + j, grp_count))
        lax.fori_loop(1, row_count, greet_row, 0)

    with scope("issue"):
        tables = [
            pltpu.make_async_copy(source, target, table_sem.at[n])
            for n, (source, target) in enumerate(
                ((list_hbm, pair_list), (count_hbm, pair_count), (blocks_hbm, pair_blocks))
            )
        ]
        sample_load = pltpu.make_async_copy(samples_hbm, samples, sample_sem)
        sample_load.start()
        for table in tables:
            table.start()
        wide = batch * width
        for i in range(LOADS):
            pltpu.make_async_copy(matrix.at[:, pl.ds(i * wide, wide)], mat.at[i], load_sem.at[min(i, FIRST_SQUARES)]).start(priority=1)

    def owner_of(k):
        other = 1 - lax.div(k, row_half)
        j = k + 1 - other
        return (top * (1 - other) + (1 - top) * other) * row_half + lax.rem(s + j, row_half)

    place_copy = pltpu.make_async_copy(place_rows, places, sample_sem)

    def fill_places():
        pair = s * region + lax.broadcasted_iota(jnp.int32, (1, place_rows.shape[1]), 1)
        for k in range(row_count):
            source = source_of(k)
            slot = jnp.full(pair.shape, cap, jnp.int32)
            for n in range(half if k < row_half else cap):
                at = high * half + n if k < row_half else n
                slot = jnp.where(pair == pair_list[source, at, s], at, slot)
            place_rows[k : k + 1, :] = slot
        place_copy.start()

    def source_of(k):
        return ((1 - top) if k < row_half else top) * row_half + lax.rem(s + k, row_half)

    def clear(j, carry):
        for q in range(CHUNKS):
            row_in[q][j, cap] = jnp.zeros((sizes[q], width), F32)
        return carry

    lax.fori_loop(0, row_count, clear, 0)

    with scope("w_samples"):
        sample_load.wait()
        for table in tables:
            table.wait()

    early = counts.shape[0]
    part = 128
    positions = lax.broadcasted_iota(jnp.int32, (rows_dev, part), 0)
    ones = jnp.ones((part, width), BF16)

    def count_owner(i, carry):
        owner = owner_of(i)
        for n in range(cap):
            first = pair_blocks[0, pair_list[s, n, owner]]
            active = (n < pair_count[s, owner]).astype(jnp.int32)
            picked = ((samples[first] + 1) * active - 1).reshape(1, sample_count)
            hits = None
            for c in range(sample_count // part):
                hit = jnp.where(positions == picked[:, c * part : (c + 1) * part], 1.0, 0.0)
                hits = hit if hits is None else hits + hit
            multiplicity = jnp.dot(hits.astype(BF16), ones, preferred_element_type=F32)
            counts[lax.rem(i, early), n] = multiplicity.astype(BF16)
        return carry

    with scope("places"):
        fill_places()
    with scope("counts"):
        lax.fori_loop(0, early, count_owner, 0)

    def square_batch(i, carry):
        for u in range(batch // 8):
            lines = []
            for m in range(8):
                values = mat[i, :, (u * 8 + m) * width : (u * 8 + m + 1) * width].astype(F32)
                lines.append(jnp.sum(values * values, axis=0, keepdims=True))
            squares[lines_from(i * batch + u * 8, 8), :] = jnp.concatenate(lines, axis=0)
        return carry

    def load_batch(i, carry):
        with scope("w_load"):
            await_bytes(mat.at[i], load_sem.at[i])
        return square_batch(i, carry)

    with scope("load_sq"):
        lax.fori_loop(0, FIRST_SQUARES, load_batch, 0)
    with scope("load_rest"):
        await_bytes(mat.at[pl.ds(FIRST_SQUARES, LOADS - FIRST_SQUARES)], load_sem.at[FIRST_SQUARES])

    nb8 = block_count // 8
    side = lax.rem(s, 2)
    seat = side * grp_count + g
    peers = [lax.rem(seat + j, 8) for j in range(1, 8)]

    def eighth(peer):
        grp = lax.rem(peer, grp_count)
        at = lax.rem(grp, 2) * 4 + lax.div(grp, 2) * 2 + lax.div(peer, grp_count)
        return lines_from(at * nb8, nb8)

    def peer_row(peer):
        return s - side + lax.div(peer, grp_count)

    def sq_first():
        for peer in peers:
            send(
                squares.at[eighth(peer)], sq_parts.at[seat], sq_send.at[0], sq_recv.at[0],
                peer_row(peer), lax.rem(peer, grp_count),
            ).start()

    def even_row(j):
        return lax.rem(s + 2 * j, row_count)

    def sq_second():
        await_bytes(sq_parts.at[pl.ds(0, 7)], sq_recv.at[0])
        total = squares[eighth(seat), :]
        for peer in peers:
            total = total + sq_parts[peer]
        sq_rows[s] = total

        def sq_row(j, carry):
            send(sq_rows.at[s], sq_rows.at[s], near_send, near_recv, even_row(j), g).start()
            return carry

        lax.fori_loop(1, row_half, sq_row, 0)

    def sq_third():
        await_bytes(sq_rows.at[pl.ds(0, row_half - 1)], near_recv)
        total = sq_rows[s]
        for j in range(1, row_half):
            total = total + sq_rows[even_row(j)]
        here = eighth(seat)
        sq_total[here, :] = total
        for peer in peers:
            send(
                sq_total.at[here], sq_total.at[here], sq_send.at[1], sq_recv.at[1],
                peer_row(peer), lax.rem(peer, grp_count),
            ).start()

    my_lines = lines_from(low * tall, tall)
    their_lines = lines_from((1 - low) * tall, tall)
    mine = pl.ds(high * half, half)
    theirs = pl.ds((1 - high) * half, half)
    every = pl.ds(0, cap)

    def lines(q):
        return lines_from(low * tall + starts[q], sizes[q])

    def within(q):
        return pl.ds(starts[q] - sizes[0], sizes[q])

    def core_copy(k):
        return send(tiles.at[k, every, their_lines], core_in.at[k], core_send, core_recv.at[k], s, partner)

    def high_copy(k, q):
        target = high_in.at[k, pl.ds(0, half), within(q)]
        arrived = high_recv.at[row_half + q - 1]
        return send(tiles.at[k, theirs, lines(q)], target, high_send, arrived, s, across)

    def first_copy(k, t):
        there = lines(0) if t == 0 else lines_from((1 - low) * tall, sizes[0])
        target = first_in.at[k, t]
        return send(tiles.at[k, theirs, there], target, first_send, high_recv.at[k], s, across if t == 0 else corner)

    def far_copy(k, q):
        return send(tiles.at[k, mine, lines(q)], row_in[q].at[s, mine], row_send, row_recv.at[q], owner_of(k), g)

    def near_copy(k, q):
        return send(tiles.at[k, every, lines(q)], row_in[q].at[s, every], row_send, row_recv.at[q], owner_of(k), g)

    def block(b):
        return mat[lax.div(b, batch), :, pl.ds(lax.rem(b, batch) * width, width)]

    def make(k):
        owner = owner_of(k)
        for n in range(cap):
            pair = pair_list[s, n, owner]
            weighted = counts[lax.rem(k, early), n] * block(pair_blocks[0, pair])
            tiles[k, n] = lax.dot_general(
                weighted, block(pair_blocks[1, pair]), (((0,), (0,)), ((), ())),
                preferred_element_type=F32,
            )

    later = lines_from(low * tall + sizes[0], tall - sizes[0])

    def fold_far(k):
        core_copy(k).wait_recv()
        tiles[k, :, later] = tiles[k, :, later] + core_in[k, :, sizes[0] :]
        high_copy(k, 1).start()

    def fold_near(k):
        core_copy(k).wait_recv()
        tiles[k, :, my_lines] = tiles[k, :, my_lines] + core_in[k]

    def cross_first(k):
        await_bytes(first_in.at[k], high_recv.at[k])
        own = tiles[k, mine, lines(0)] + core_in[k, mine, 0 : sizes[0]]
        tiles[k, mine, lines(0)] = own + (first_in[k, 0] + first_in[k, 1])
        far_copy(k, 0).start()

    def cross(k, q):
        tiles[k, mine, lines(q)] = tiles[k, mine, lines(q)] + high_in[k, :, within(q)]
        far_copy(k, q).start()

    def produce(k):
        if early < row_count:
            @pl.when(k >= early)
            def _():
                with scope("count"):
                    count_owner(k, 0)

        with scope("make"):
            make(k)

    def deliver(k):
        core_copy(k).start()
        for t in range(2):
            first_copy(k, t).start()

    def high_go(q):
        def go(k, carry):
            high_copy(k, q).start()
            return carry

        lax.fori_loop(0, row_half, go, 0)

    produce(0)
    with scope("barrier"):
        pl.semaphore_wait(barrier, row_count + 5)
    deliver(0)

    def far_step(k, carry):
        produce(k)
        deliver(k)
        return carry

    def near_step(j, carry):
        produce(row_half + j)
        core_copy(row_half + j).start()
        with scope("fold"):
            fold_far(j)
        return carry

    def sum_step(j, carry):
        with scope("cross0"):
            cross_first(j)
        with scope("fold"):
            fold_near(row_half + j)

        @pl.when(row_half + j < last)
        def _():
            near_copy(row_half + j, 0).start()

        @pl.when(FIRST_SQUARES + j < LOADS)
        def _():
            with scope("squares"):
                square_batch(FIRST_SQUARES + j, 0)

        return carry

    lax.fori_loop(1, row_half, far_step, 0)
    lax.fori_loop(0, row_half, near_step, 0)
    @pl.when(low == 0)
    def _():
        high_go(2)

    lax.fori_loop(0, row_half, sum_step, 0)

    @pl.when(low == 1)
    def _():
        high_go(2)

    with scope("squares"):
        lax.fori_loop(min(FIRST_SQUARES + row_half, LOADS), LOADS, square_batch, 0)
    sq_first()
    for q in range(3, CHUNKS):
        high_go(q)

    def crosses(q):
        def near_go(k, carry):
            near_copy(k, q).start()
            return carry

        def cross_go(k, carry):
            cross(k, q)
            return carry

        with scope("crosses"):
            @pl.when(low == 0)
            def _():
                lax.fori_loop(row_half, last, near_go, 0)

            await_bytes(high_in.at[:, :, within(q)], high_recv.at[row_half + q - 1])
            lax.fori_loop(0, row_half, cross_go, 0)

            @pl.when(low == 1)
            def _():
                lax.fori_loop(row_half, last, near_go, 0)

    crosses(1)
    crosses(2)
    for q in range(CHUNKS):
        row_in[q][s, every] = tiles[last, :, lines(q)]

    def owned(q, grp, n):
        j = grp * tile_dev + n
        total = row_in[q][source_of(0), places[0, j]]
        for k in range(1, row_count):
            total = total + row_in[q][source_of(k), places[k, j]]
        return total

    distant = ((1 - high) * 2 + (1 - low), (1 - high) * 2 + low)
    local = (partner, g)

    def b_copy(q, t):
        return send(part_b[q].at[t], in_b[q].at[t], b_send, b_recv.at[q if q < CHUNKS - 1 else q + t], s, across)

    def c_copy(q):
        return send(part_c[q], in_c[q], c_send, c_recv.at[q], s, partner)

    arriving = 3 * row_count // 4 - 1

    def post(q):
        with scope("w_rows"):
            await_bytes(row_in[q].at[pl.ds(0, arriving), every], row_recv.at[q])
        with scope("post"):
            for t in range(2):
                def away(n, carry):
                    part_b[q][t, n] = owned(q, distant[t], n)
                    return carry

                lax.fori_loop(0, tile_dev, away, 0)
                b_copy(q, t).start()
            for t in range(2):
                def hold(n, carry):
                    held[q][t, n] = owned(q, local[t], n)
                    return carry

                lax.fori_loop(0, tile_dev, hold, 0)

    def store(place, values, scaled):
        out[:, place] = values * scale[:, place] if scaled else values

    def finish(q, scaled=False):
        with scope("w_b0"):
            if q < CHUNKS - 1:
                await_bytes(in_b[q], b_recv.at[q])
            else:
                b_copy(q, 0).wait_recv()
        part_c[q][...] = held[q][0] + in_b[q][0]
        c_copy(q).start()
        if q == CHUNKS - 1:
            with scope("w_b1"):
                b_copy(q, 1).wait_recv()
        store(lines(q), held[q][1] + in_b[q][1], scaled)

    def collect(q, scaled=False):
        with scope("w_c"):
            c_copy(q).wait_recv()
        store(lines_from((1 - low) * tall + starts[q], sizes[q]), in_c[q][...], scaled)

    def factors():
        await_bytes(sq_total.at[pl.ds(0, 7 * nb8)], sq_recv.at[1])
        await_bytes(sq_parts.at[pl.ds(0, 7)], sq_send.at[1])
        sq_total[...] = jnp.sqrt(sq_total[...] / (rows_dev * row_count * grp_count) + epsilon)

        def factor(n, carry):
            pair = (s * region + g * tile_dev) + n
            left = sq_total[pair_blocks[0, pair]].reshape(1, width)
            right = sq_total[pair_blocks[1, pair]].reshape(1, width)
            left = jnp.broadcast_to(left, (width, width)).T
            scale[n] = 1.0 / (sample_count * left * right)
            return carry

        lax.fori_loop(0, tile_dev, factor, 0)

    def rescale(start, size):
        piece = lines_from(start, size)
        out[:, piece] = out[:, piece] * scale[:, piece]

    with scope("w_places"):
        place_copy.wait()
    post(0)
    with scope("sq_second"):
        sq_second()
    for q in range(3, CHUNKS):
        crosses(q)
    post(1)
    finish(0)
    post(2)
    with scope("sq_third"):
        sq_third()
    finish(1)
    collect(0)
    for q in range(3, CHUNKS):
        post(q)
        finish(q - 1)
        collect(q - 2)
    with scope("factors"):
        factors()
    rescale(low * tall, starts[CHUNKS - 1])
    rescale((1 - low) * tall, starts[CHUNKS - 2])
    finish(CHUNKS - 1, True)
    collect(CHUNKS - 2, True)
    collect(CHUNKS - 1, True)

    with scope("drain"):
        await_bytes(core_in, core_send)
        await_bytes(first_in, first_send)
        await_bytes(high_in, high_send)
        await_bytes(tiles.at[pl.ds(0, arriving), every, pl.ds(0, tall)], row_send)
        await_bytes(tiles.at[pl.ds(0, tile_dev // cap), every, pl.ds(0, tall)], c_send)
        await_bytes(tiles.at[pl.ds(0, 2 * tile_dev // cap), every, pl.ds(0, tall)], b_send)
        await_bytes(sq_rows.at[pl.ds(0, row_half - 1)], near_send)
        await_bytes(sq_parts.at[pl.ds(0, 7)], sq_send.at[0])


def shards(matrix, sample_rows, pair_list, pair_count, pair_blocks):
    rows_dev, column_count = matrix.shape
    block_count, sample_count = sample_rows.shape[1:]
    width = column_count // block_count
    row_count = lax.axis_size("rows")
    grp_count = lax.axis_size("grp")
    cap = pair_list.shape[2]
    pairs = pair_blocks.shape[0]
    region = pairs // row_count
    tile_dev = region // grp_count
    half = cap // 2
    row_half = row_count // 2
    tall = width // 2
    sizes = [share * tall // sum(SHARES) for share in SHARES]
    nb8 = block_count // 8
    early = min(row_count, EARLY)
    dma = pltpu.SemaphoreType.DMA

    def vmem(*shape):
        return pltpu.VMEM(shape, F32)

    def smem(*shape):
        return pltpu.SMEM(shape, jnp.int32)

    dims = (row_count, grp_count, cap, pairs, block_count, width)
    return pl.pallas_call(
        functools.partial(kernel, dims),
        out_shape=pltpu.VMEM((tile_dev, width, width), F32),
        in_specs=[pl.BlockSpec(memory_space=pl.ANY) for _ in range(5)],
        out_specs=pl.BlockSpec(memory_space=pltpu.VMEM),
        scratch_shapes=[
            pltpu.VMEM((LOADS, rows_dev, column_count // LOADS), BF16),
            pltpu.VMEM((block_count, sample_count), jnp.int32),
            pltpu.VMEM((early, cap, rows_dev, width), BF16),
            smem(row_count, 128),
            vmem(row_count, cap, width, width),
            vmem(row_count, cap, tall, width),
            vmem(row_half, half, tall - sizes[0], width),
            vmem(row_half, 2, half, sizes[0], width),
            *[vmem(row_count, cap + 1, size, width) for size in sizes],
            *[vmem(2, tile_dev, size, width) for size in sizes],
            *[vmem(2, tile_dev, size, width) for size in sizes],
            *[vmem(2, tile_dev, size, width) for size in sizes],
            *[vmem(tile_dev, size, width) for size in sizes],
            *[vmem(tile_dev, size, width) for size in sizes],
            pltpu.VMEM((row_count, 128), jnp.int32),
            vmem(tile_dev, width, width),
            vmem(block_count, width), vmem(8, nb8, width), vmem(row_count, nb8, width),
            vmem(block_count, width),
            smem(row_count, cap, row_count), smem(row_count, row_count), smem(2, pairs),
            dma((3,)), dma, dma((FIRST_SQUARES + 1,)), dma((2,)), dma((2,)), dma, dma, dma, dma((row_count,)),
            dma, dma, dma((row_half + CHUNKS - 1,)), dma, dma((CHUNKS,)),
            dma, dma((CHUNKS + 1,)), dma, dma((CHUNKS,)),
        ],
        compiler_params=pltpu.CompilerParams(
            collective_id=0, has_side_effects=True, vmem_limit_bytes=60000000
        ),
        name="gram_tiles",
    )(pair_list.transpose(0, 2, 1), pair_count, pair_blocks.T, sample_rows[0], matrix)


def solution(mesh):
    in_specs = (P(("rows", "grp"), None), P(("rows", "grp"), None, None), P(), P(), P())
    out_specs = P(("rows", "grp"), None, None)
    return jax.shard_map(shards, mesh=mesh, in_specs=in_specs, out_specs=out_specs, check_vma=False)
```

```python
import functools

import jax
import jax.numpy as jnp
from jax import lax
from jax.experimental import pallas as pl
from jax.experimental.pallas import tpu as pltpu
from jax.sharding import PartitionSpec as P

epsilon = 1e-06
MESH = pl.DeviceIdType.MESH
F32 = jnp.float32
BF16 = jnp.bfloat16
SHARES = (2, 2, 2, 2)
CHUNKS = len(SHARES)
LOADS = 8
EARLY = 8
FIRST_SQUARES = 2
scope = jax.named_scope


def kernel(
    dims, list_hbm, count_hbm, blocks_hbm, samples_hbm, matrix, out, *scratch,
):
    row_count, grp_count, cap, pairs, block_count, width = dims
    it = iter(scratch)
    mat, samples, counts, places, tiles, core_in, high_in, first_in = [next(it) for _ in range(8)]
    row_in, part_b, in_b, held, part_c, in_c = [[next(it) for _ in range(CHUNKS)] for _ in range(6)]
    place_rows, scale, squares, sq_parts, sq_rows, sq_total = [next(it) for _ in range(6)]
    pair_list, pair_count, pair_blocks = [next(it) for _ in range(3)]
    (table_sem, sample_sem, load_sem, sq_send, sq_recv, near_send, near_recv, core_send, core_recv,
     first_send, high_send, high_recv, row_send, row_recv, b_send, b_recv, c_send, c_recv) = it

    batch = block_count // LOADS
    rows_dev = mat.shape[1]
    sample_count = samples.shape[1]
    half = cap // 2
    region = pairs // row_count
    tile_dev = region // grp_count
    row_half = row_count // 2
    tall = width // 2
    sizes = [share * tall // sum(SHARES) for share in SHARES]
    starts = [sum(sizes[:q]) for q in range(CHUNKS)]
    last = row_count - 1

    s = lax.axis_index("rows")
    g = lax.axis_index("grp")
    low = lax.rem(g, 2)
    high = lax.div(g, 2)
    partner = high * 2 + (1 - low)
    across = (1 - high) * 2 + low
    corner = (1 - high) * 2 + (1 - low)
    top = lax.div(s, row_half)

    def send(source, target, send_sem, recv_sem, row, grp):
        return pltpu.make_async_remote_copy(
            src_ref=source, dst_ref=target, send_sem=send_sem, recv_sem=recv_sem,
            device_id={"rows": row, "grp": grp}, device_id_type=MESH,
        )

    def await_bytes(ref, sem):
        pltpu.make_async_copy(ref, ref, sem).wait()

    def lines_from(start, size):
        return pl.ds(pl.multiple_of(start, 8), size)

    with scope("greet"):
        barrier = pltpu.get_barrier_semaphore()

        def greet(row, grp):
            pl.semaphore_signal(barrier, inc=1, device_id={"rows": row, "grp": grp}, device_id_type=MESH)

        def greet_row(j, carry):
            greet(lax.rem(s + j, row_count), g)
            return carry

        greet(s, partner)
        greet(s, across)
        greet(s, corner)
        for j in range(1, grp_count):
            greet(s + 1 - 2 * lax.rem(s, 2), lax.rem(g + j, grp_count))
        lax.fori_loop(1, row_count, greet_row, 0)

    with scope("issue"):
        tables = [
            pltpu.make_async_copy(source, target, table_sem.at[n])
            for n, (source, target) in enumerate(
                ((list_hbm, pair_list), (count_hbm, pair_count), (blocks_hbm, pair_blocks))
            )
        ]
        sample_load = pltpu.make_async_copy(samples_hbm, samples, sample_sem)
        sample_load.start()
        for table in tables:
            table.start()
        wide = batch * width
        for i in range(LOADS):
            pltpu.make_async_copy(matrix.at[:, pl.ds(i * wide, wide)], mat.at[i], load_sem.at[min(i, FIRST_SQUARES)]).start(priority=1)

    def owner_of(k):
        other = 1 - lax.div(k, row_half)
        j = k + 1 - other
        return (top * (1 - other) + (1 - top) * other) * row_half + lax.rem(s + j, row_half)

    place_copy = pltpu.make_async_copy(place_rows, places, sample_sem)

    def fill_places():
        pair = s * region + lax.broadcasted_iota(jnp.int32, (1, place_rows.shape[1]), 1)
        for k in range(row_count):
            source = source_of(k)
            slot = jnp.full(pair.shape, cap, jnp.int32)
            for n in range(half if k < row_half else cap):
                at = high * half + n if k < row_half else n
                slot = jnp.where(pair == pair_list[source, at, s], at, slot)
            place_rows[k : k + 1, :] = slot
        place_copy.start()

    def source_of(k):
        return ((1 - top) if k < row_half else top) * row_half + lax.rem(s + k, row_half)

    def clear(j, carry):
        for q in range(CHUNKS):
            row_in[q][j, cap] = jnp.zeros((sizes[q], width), F32)
        return carry

    lax.fori_loop(0, row_count, clear, 0)

    with scope("w_samples"):
        sample_load.wait()
        for table in tables:
            table.wait()

    early = counts.shape[0]
    part = 128
    positions = lax.broadcasted_iota(jnp.int32, (rows_dev, part), 0)
    ones = jnp.ones((part, width), BF16)

    def count_owner(i, carry):
        owner = owner_of(i)
        for n in range(cap):
            first = pair_blocks[0, pair_list[s, n, owner]]
            active = (n < pair_count[s, owner]).astype(jnp.int32)
            picked = ((samples[first] + 1) * active - 1).reshape(1, sample_count)
            hits = None
            for c in range(sample_count // part):
                hit = jnp.where(positions == picked[:, c * part : (c + 1) * part], 1.0, 0.0)
                hits = hit if hits is None else hits + hit
            multiplicity = jnp.dot(hits.astype(BF16), ones, preferred_element_type=F32)
            counts[lax.rem(i, early), n] = multiplicity.astype(BF16)
        return carry

    with scope("places"):
        fill_places()
    with scope("counts"):
        lax.fori_loop(0, early, count_owner, 0)

    def square_batch(i, carry):
        for u in range(batch // 8):
            lines = []
            for m in range(8):
                values = mat[i, :, (u * 8 + m) * width : (u * 8 + m + 1) * width].astype(F32)
                lines.append(jnp.sum(values * values, axis=0, keepdims=True))
            squares[lines_from(i * batch + u * 8, 8), :] = jnp.concatenate(lines, axis=0)
        return carry

    def load_batch(i, carry):
        with scope("w_load"):
            await_bytes(mat.at[i], load_sem.at[i])
        return square_batch(i, carry)

    with scope("load_sq"):
        lax.fori_loop(0, FIRST_SQUARES, load_batch, 0)
    with scope("load_rest"):
        await_bytes(mat.at[pl.ds(FIRST_SQUARES, LOADS - FIRST_SQUARES)], load_sem.at[FIRST_SQUARES])

    nb8 = block_count // 8
    side = lax.rem(s, 2)
    seat = side * grp_count + g
    peers = [lax.rem(seat + j, 8) for j in range(1, 8)]

    def eighth(peer):
        grp = lax.rem(peer, grp_count)
        at = lax.rem(grp, 2) * 4 + lax.div(grp, 2) * 2 + lax.div(peer, grp_count)
        return lines_from(at * nb8, nb8)

    def peer_row(peer):
        return s - side + lax.div(peer, grp_count)

    def sq_first():
        for peer in peers:
            send(
                squares.at[eighth(peer)], sq_parts.at[seat], sq_send.at[0], sq_recv.at[0],
                peer_row(peer), lax.rem(peer, grp_count),
            ).start()

    def even_row(j):
        return lax.rem(s + 2 * j, row_count)

    def sq_second():
        await_bytes(sq_parts.at[pl.ds(0, 7)], sq_recv.at[0])
        total = squares[eighth(seat), :]
        for peer in peers:
            total = total + sq_parts[peer]
        sq_rows[s] = total

        def sq_row(j, carry):
            send(sq_rows.at[s], sq_rows.at[s], near_send, near_recv, even_row(j), g).start()
            return carry

        lax.fori_loop(1, row_half, sq_row, 0)

    def sq_third():
        await_bytes(sq_rows.at[pl.ds(0, row_half - 1)], near_recv)
        total = sq_rows[s]
        for j in range(1, row_half):
            total = total + sq_rows[even_row(j)]
        here = eighth(seat)
        sq_total[here, :] = total
        for peer in peers:
            send(
                sq_total.at[here], sq_total.at[here], sq_send.at[1], sq_recv.at[1],
                peer_row(peer), lax.rem(peer, grp_count),
            ).start()

    my_lines = lines_from(low * tall, tall)
    their_lines = lines_from((1 - low) * tall, tall)
    mine = pl.ds(high * half, half)
    theirs = pl.ds((1 - high) * half, half)
    every = pl.ds(0, cap)

    def lines(q):
        return lines_from(low * tall + starts[q], sizes[q])

    def within(q):
        return pl.ds(starts[q] - sizes[0], sizes[q])

    def core_copy(k):
        return send(tiles.at[k, every, their_lines], core_in.at[k], core_send, core_recv.at[k], s, partner)

    def high_copy(k, q):
        target = high_in.at[k, pl.ds(0, half), within(q)]
        arrived = high_recv.at[row_half + q - 1]
        return send(tiles.at[k, theirs, lines(q)], target, high_send, arrived, s, across)

    def first_copy(k, t):
        there = lines(0) if t == 0 else lines_from((1 - low) * tall, sizes[0])
        target = first_in.at[k, t]
        return send(tiles.at[k, theirs, there], target, first_send, high_recv.at[k], s, across if t == 0 else corner)

    def far_copy(k, q):
        return send(tiles.at[k, mine, lines(q)], row_in[q].at[s, mine], row_send, row_recv.at[q], owner_of(k), g)

    def near_copy(k, q):
        return send(tiles.at[k, every, lines(q)], row_in[q].at[s, every], row_send, row_recv.at[q], owner_of(k), g)

    def block(b):
        return mat[lax.div(b, batch), :, pl.ds(lax.rem(b, batch) * width, width)]

    def make(k):
        owner = owner_of(k)
        for n in range(cap):
            pair = pair_list[s, n, owner]
            weighted = counts[lax.rem(k, early), n] * block(pair_blocks[0, pair])
            tiles[k, n] = lax.dot_general(
                weighted, block(pair_blocks[1, pair]), (((0,), (0,)), ((), ())),
                preferred_element_type=F32,
            )

    later = lines_from(low * tall + sizes[0], tall - sizes[0])

    def fold_far(k):
        core_copy(k).wait_recv()
        tiles[k, :, later] = tiles[k, :, later] + core_in[k, :, sizes[0] :]
        high_copy(k, 1).start()

    def fold_near(k):
        core_copy(k).wait_recv()
        tiles[k, :, my_lines] = tiles[k, :, my_lines] + core_in[k]

    def cross_first(k):
        await_bytes(first_in.at[k], high_recv.at[k])
        own = tiles[k, mine, lines(0)] + core_in[k, mine, 0 : sizes[0]]
        tiles[k, mine, lines(0)] = own + (first_in[k, 0] + first_in[k, 1])
        far_copy(k, 0).start()

    def cross(k, q):
        tiles[k, mine, lines(q)] = tiles[k, mine, lines(q)] + high_in[k, :, within(q)]
        far_copy(k, q).start()

    def produce(k):
        if early < row_count:
            @pl.when(k >= early)
            def _():
                with scope("count"):
                    count_owner(k, 0)

        with scope("make"):
            make(k)

    def deliver(k):
        core_copy(k).start()
        for t in range(2):
            first_copy(k, t).start()

    def high_go(q):
        def go(k, carry):
            high_copy(k, q).start()
            return carry

        lax.fori_loop(0, row_half, go, 0)

    produce(0)
    with scope("barrier"):
        pl.semaphore_wait(barrier, row_count + 5)
    deliver(0)

    def far_step(k, carry):
        produce(k)
        deliver(k)
        return carry

    def near_step(j, carry):
        produce(row_half + j)
        core_copy(row_half + j).start()
        with scope("fold"):
            fold_far(j)
        return carry

    def sum_step(j, carry):
        with scope("cross0"):
            cross_first(j)
        with scope("fold"):
            fold_near(row_half + j)

        @pl.when(row_half + j < last)
        def _():
            near_copy(row_half + j, 0).start()

        @pl.when(FIRST_SQUARES + j < LOADS)
        def _():
            with scope("squares"):
                square_batch(FIRST_SQUARES + j, 0)

        return carry

    lax.fori_loop(1, row_half, far_step, 0)
    lax.fori_loop(0, row_half, near_step, 0)
    @pl.when(low == 0)
    def _():
        high_go(2)

    lax.fori_loop(0, row_half, sum_step, 0)

    @pl.when(low == 1)
    def _():
        high_go(2)

    with scope("squares"):
        lax.fori_loop(min(FIRST_SQUARES + row_half, LOADS), LOADS, square_batch, 0)
    sq_first()
    for q in range(3, CHUNKS):
        high_go(q)

    def crosses(q):
        def near_go(k, carry):
            near_copy(k, q).start()
            return carry

        def cross_go(k, carry):
            cross(k, q)
            return carry

        with scope("crosses"):
            @pl.when(low == 0)
            def _():
                lax.fori_loop(row_half, last, near_go, 0)

            await_bytes(high_in.at[:, :, within(q)], high_recv.at[row_half + q - 1])
            lax.fori_loop(0, row_half, cross_go, 0)

            @pl.when(low == 1)
            def _():
                lax.fori_loop(row_half, last, near_go, 0)

    crosses(1)
    crosses(2)
    for q in range(CHUNKS):
        row_in[q][s, every] = tiles[last, :, lines(q)]

    def owned(q, grp, n):
        j = grp * tile_dev + n
        total = row_in[q][source_of(0), places[0, j]]
        for k in range(1, row_count):
            total = total + row_in[q][source_of(k), places[k, j]]
        return total

    distant = ((1 - high) * 2 + (1 - low), (1 - high) * 2 + low)
    local = (partner, g)

    def b_copy(q, t, which):
        return send(part_b[q].at[t, which], in_b[q].at[t, which], b_send, b_recv.at[q if q < CHUNKS - 1 else q + t], s, across)

    def c_copy(q):
        return send(part_c[q], in_c[q], c_send, c_recv.at[q], s, partner)

    arriving = 3 * row_count // 4 - 1

    def post(q):
        with scope("w_rows"):
            await_bytes(row_in[q].at[pl.ds(0, arriving), every], row_recv.at[q])
        with scope("post"):
            for t in range(2):
                def away(n, carry):
                    part_b[q][t, n] = owned(q, distant[t], n)
                    return carry

                pieces = 2 if q == CHUNKS - 1 else 1
                for c in range(pieces):
                    size = tile_dev // pieces
                    lax.fori_loop(c * size, (c + 1) * size, away, 0)
                    b_copy(q, t, pl.ds(c * size, size)).start()
            for t in range(2):
                def hold(n, carry):
                    held[q][t, n] = owned(q, local[t], n)
                    return carry

                lax.fori_loop(0, tile_dev, hold, 0)

    def store(place, values, scaled):
        out[:, place] = values * scale[:, place] if scaled else values

    def finish(q, scaled=False):
        with scope("w_b0"):
            if q < CHUNKS - 1:
                await_bytes(in_b[q], b_recv.at[q])
            else:
                await_bytes(in_b[q].at[0], b_recv.at[q])
        part_c[q][...] = held[q][0] + in_b[q][0]
        c_copy(q).start()
        if q == CHUNKS - 1:
            with scope("w_b1"):
                await_bytes(in_b[q].at[1], b_recv.at[q + 1])
        store(lines(q), held[q][1] + in_b[q][1], scaled)

    def collect(q, scaled=False):
        with scope("w_c"):
            c_copy(q).wait_recv()
        store(lines_from((1 - low) * tall + starts[q], sizes[q]), in_c[q][...], scaled)

    def factors():
        await_bytes(sq_total.at[pl.ds(0, 7 * nb8)], sq_recv.at[1])
        await_bytes(sq_parts.at[pl.ds(0, 7)], sq_send.at[1])
        sq_total[...] = jnp.sqrt(sq_total[...] / (rows_dev * row_count * grp_count) + epsilon)

        def factor(n, carry):
            pair = (s * region + g * tile_dev) + n
            left = sq_total[pair_blocks[0, pair]].reshape(1, width)
            right = sq_total[pair_blocks[1, pair]].reshape(1, width)
            left = jnp.broadcast_to(left, (width, width)).T
            scale[n] = 1.0 / (sample_count * left * right)
            return carry

        lax.fori_loop(0, tile_dev, factor, 0)

    def rescale(start, size):
        piece = lines_from(start, size)
        out[:, piece] = out[:, piece] * scale[:, piece]

    with scope("w_places"):
        place_copy.wait()
    post(0)
    with scope("sq_second"):
        sq_second()
    for q in range(3, CHUNKS):
        crosses(q)
    post(1)
    finish(0)
    post(2)
    with scope("sq_third"):
        sq_third()
    finish(1)
    collect(0)
    for q in range(3, CHUNKS):
        post(q)
        finish(q - 1)
        collect(q - 2)
    with scope("factors"):
        factors()
    rescale(low * tall, starts[CHUNKS - 1])
    rescale((1 - low) * tall, starts[CHUNKS - 2])
    finish(CHUNKS - 1, True)
    collect(CHUNKS - 2, True)
    collect(CHUNKS - 1, True)

    with scope("drain"):
        await_bytes(core_in, core_send)
        await_bytes(first_in, first_send)
        await_bytes(high_in, high_send)
        await_bytes(tiles.at[pl.ds(0, arriving), every, pl.ds(0, tall)], row_send)
        await_bytes(tiles.at[pl.ds(0, tile_dev // cap), every, pl.ds(0, tall)], c_send)
        await_bytes(tiles.at[pl.ds(0, 2 * tile_dev // cap), every, pl.ds(0, tall)], b_send)
        await_bytes(sq_rows.at[pl.ds(0, row_half - 1)], near_send)
        await_bytes(sq_parts.at[pl.ds(0, 7)], sq_send.at[0])


def shards(matrix, sample_rows, pair_list, pair_count, pair_blocks):
    rows_dev, column_count = matrix.shape
    block_count, sample_count = sample_rows.shape[1:]
    width = column_count // block_count
    row_count = lax.axis_size("rows")
    grp_count = lax.axis_size("grp")
    cap = pair_list.shape[2]
    pairs = pair_blocks.shape[0]
    region = pairs // row_count
    tile_dev = region // grp_count
    half = cap // 2
    row_half = row_count // 2
    tall = width // 2
    sizes = [share * tall // sum(SHARES) for share in SHARES]
    nb8 = block_count // 8
    early = min(row_count, EARLY)
    dma = pltpu.SemaphoreType.DMA

    def vmem(*shape):
        return pltpu.VMEM(shape, F32)

    def smem(*shape):
        return pltpu.SMEM(shape, jnp.int32)

    dims = (row_count, grp_count, cap, pairs, block_count, width)
    return pl.pallas_call(
        functools.partial(kernel, dims),
        out_shape=pltpu.VMEM((tile_dev, width, width), F32),
        in_specs=[pl.BlockSpec(memory_space=pl.ANY) for _ in range(5)],
        out_specs=pl.BlockSpec(memory_space=pltpu.VMEM),
        scratch_shapes=[
            pltpu.VMEM((LOADS, rows_dev, column_count // LOADS), BF16),
            pltpu.VMEM((block_count, sample_count), jnp.int32),
            pltpu.VMEM((early, cap, rows_dev, width), BF16),
            smem(row_count, 128),
            vmem(row_count, cap, width, width),
            vmem(row_count, cap, tall, width),
            vmem(row_half, half, tall - sizes[0], width),
            vmem(row_half, 2, half, sizes[0], width),
            *[vmem(row_count, cap + 1, size, width) for size in sizes],
            *[vmem(2, tile_dev, size, width) for size in sizes],
            *[vmem(2, tile_dev, size, width) for size in sizes],
            *[vmem(2, tile_dev, size, width) for size in sizes],
            *[vmem(tile_dev, size, width) for size in sizes],
            *[vmem(tile_dev, size, width) for size in sizes],
            pltpu.VMEM((row_count, 128), jnp.int32),
            vmem(tile_dev, width, width),
            vmem(block_count, width), vmem(8, nb8, width), vmem(row_count, nb8, width),
            vmem(block_count, width),
            smem(row_count, cap, row_count), smem(row_count, row_count), smem(2, pairs),
            dma((3,)), dma, dma((FIRST_SQUARES + 1,)), dma((2,)), dma((2,)), dma, dma, dma, dma((row_count,)),
            dma, dma, dma((row_half + CHUNKS - 1,)), dma, dma((CHUNKS,)),
            dma, dma((CHUNKS + 1,)), dma, dma((CHUNKS,)),
        ],
        compiler_params=pltpu.CompilerParams(
            collective_id=0, has_side_effects=True, vmem_limit_bytes=60000000
        ),
        name="gram_tiles",
    )(pair_list.transpose(0, 2, 1), pair_count, pair_blocks.T, sample_rows[0], matrix)


def solution(mesh):
    in_specs = (P(("rows", "grp"), None), P(("rows", "grp"), None, None), P(), P(), P())
    out_specs = P(("rows", "grp"), None, None)
    return jax.shard_map(shards, mesh=mesh, in_specs=in_specs, out_specs=out_specs, check_vma=False)
```
